64 devices in a mesh: member: 4 (over x, y), lat: 16 (over z, core).
Axes of the slice: x: 2, y: 2, z: 8, core: 2. Of those that a mesh axis runs over, the one named last changes fastest.
The devices are a block of a 4x4x8 slice.
Arguments:
- field: float32 [512, 256, 512], P('member', 'lat'), parts along dimension 0
- p_fwd: float32 [256, 256, 256], replicated
- p_inv: float32 [256, 256, 256], replicated
- w_mix: float32 [256, 128, 128, 2], replicated
Outputs:
- output: float32 [512, 256, 512], P('member', 'lat'), parts along dimension 0
There are 4 independent parts. The reference program is written for one: setup_inputs(seed, part) draws one part's arguments, and reference() takes and returns one part's arrays. A program takes and returns all parts, laid end to end along the dimension named above; an argument that names none is the same for every part.
All inputs are finite; a program needn't handle non-finite values.
Results may differ from the reference program's by a relative error of at most 0.0116587.
Values are sent between devices in bfloat16 or wider.
A program may use at most 768 MiB of HBM per device.

```python
import jax
import jax.numpy as jnp
from jax import lax

CHANNELS = 128
N_LAT = 256
L_MAX = 256
N_LON = 2 * N_LAT


def setup_inputs(seed: int = 0, part: int = 0) -> dict:
    base_key = jax.random.key(seed)
    field_key = jax.random.fold_in(jax.random.fold_in(base_key, 1), part)
    fwd_key, inv_key, mix_key = jax.random.split(jax.random.fold_in(base_key, 2), 3)
    tri_mask = jnp.arange(L_MAX)[None, :, None] >= jnp.arange(L_MAX)[:, None, None]
    field = jax.random.normal(field_key, (CHANNELS, N_LAT, N_LON), jnp.float32)
    fwd_scale = (2.0 / (N_LAT * N_LON)) ** 0.5
    inv_scale = 1.0 / L_MAX
    mix_scale = (0.5 / CHANNELS) ** 0.5
    p_fwd = jnp.where(tri_mask, jax.random.normal(fwd_key, (L_MAX, L_MAX, N_LAT), jnp.float32) * fwd_scale, 0.0)
    p_inv = jnp.where(tri_mask, jax.random.normal(inv_key, (L_MAX, L_MAX, N_LAT), jnp.float32) * inv_scale, 0.0)
    w_mix = jax.random.normal(mix_key, (L_MAX, CHANNELS, CHANNELS, 2), jnp.float32) * mix_scale
    return {"field": field, "p_fwd": p_fwd, "p_inv": p_inv, "w_mix": w_mix}


def reference(field, p_fwd, p_inv, w_mix):
    spec_full = jnp.fft.rfft(field, axis=-1)[:, :, :L_MAX]
    spec_re = jnp.real(spec_full).astype(jnp.bfloat16).astype(jnp.float32)
    spec_im = jnp.imag(spec_full).astype(jnp.bfloat16).astype(jnp.float32)
    coef_re = jnp.einsum("mlt,ctm->clm", p_fwd, spec_re)
    coef_im = jnp.einsum("mlt,ctm->clm", p_fwd, spec_im)
    w_re = w_mix[..., 0]
    w_im = w_mix[..., 1]
    mix_re = jnp.einsum("leo,elm->olm", w_re, coef_re) - jnp.einsum("leo,elm->olm", w_im, coef_im)
    mix_im = jnp.einsum("leo,elm->olm", w_im, coef_re) + jnp.einsum("leo,elm->olm", w_re, coef_im)
    back_re = jnp.einsum("mlt,clm->ctm", p_inv, mix_re).astype(jnp.bfloat16).astype(jnp.float32)
    back_im = jnp.einsum("mlt,clm->ctm", p_inv, mix_im).astype(jnp.bfloat16).astype(jnp.float32)
    pad_cfg = ((0, 0), (0, 0), (0, N_LAT + 1 - L_MAX))
    back_cplx = lax.complex(jnp.pad(back_re, pad_cfg), jnp.pad(back_im, pad_cfg))
    wave_out = jnp.fft.irfft(back_cplx, n=N_LON, axis=-1) * N_LON
    return field + jax.nn.gelu(wave_out)
```

```python
import functools
import math

import jax
import jax.numpy as jnp
import numpy as np
from jax import lax
from jax.experimental import pallas as pl
from jax.experimental.pallas import tpu as pltpu
from jax.sharding import PartitionSpec as P

MESH = pl.DeviceIdType.MESH
F32 = jnp.float32
BF16 = jnp.bfloat16
LANES = 128
N_CHUNK = 4


def wave_tables(n_lon, groups, per_dev, n_chunk):
    piece = per_dev // n_chunk
    chunk, dev, part, k = np.meshgrid(np.arange(n_chunk), np.arange(groups), np.arange(2), np.arange(piece), indexing="ij")
    wave = ((chunk * piece + k) * groups + dev).reshape(-1, 1)
    part = part.reshape(-1, 1)
    angle = ((wave * np.arange(n_lon)[None, :]) % n_lon) * (2.0 * math.pi / n_lon)
    fwd = np.where(part == 0, np.cos(angle), -np.sin(angle)).astype(np.float32)
    inv = fwd * np.where(wave == 0, 1.0, 2.0).astype(np.float32)
    return jnp.asarray(fwd, BF16), jnp.asarray(inv, BF16)


def dot(a, b, dims):
    return lax.dot_general(a, b, (dims, ((), ())), preferred_element_type=F32)


def layer_kernel(dims, f_hbm, pw_hbm, pi_hbm, w_hbm, tf_hbm, ti_hbm, o_hbm,
                 f_v, h_v, w_v, stage, pw_v, pi_v, f_send, f_recv, g_send, g_recv, wide, coef, tf_v, ti_v,
                 in_sem, f_sem, pw_sem, pi_sem, w_sem, own_sem, fs_sem, fr_sem, gs_sem, gr_sem):
    groups, n_chan, lat_loc, n_lon, l_max, n_lat, n_chunk = dims
    per_dev = l_max // groups
    piece = per_dev // n_chunk
    rows = 2 * piece
    block = lat_loc * rows
    l_step = l_max // n_chunk
    member, me = lax.axis_index("member"), lax.axis_index("lat")
    n_z = groups // 2
    z, core = me // 2, lax.rem(me, 2)

    def peer(i):
        step = i // 2
        dist = n_z // 2 - (step + 1) // 2
        dz = jnp.where(lax.rem(step, 2) == 1, dist, -dist)
        far = lax.rem(z + dz + n_z, n_z) * 2 + lax.rem(i, 2)
        return jnp.where(i == groups - 2, z * 2 + 1 - core, far)

    barrier = pltpu.get_barrier_semaphore()

    def greet(i, _):
        pl.semaphore_signal(barrier, inc=1, device_id=(member, peer(i)), device_id_type=MESH)
        return 0

    lax.fori_loop(0, groups - 1, greet, 0)

    n_col = n_lon // LANES

    def f_in(x):
        return pltpu.make_async_copy(f_hbm.at[:, pl.ds(x * LANES, LANES)], f_v.at[x], f_sem.at[x])

    def f_out(x):
        return pltpu.make_async_copy(f_v.at[x], o_hbm.at[:, pl.ds(x * LANES, LANES)], f_sem.at[x])

    tf_in = pltpu.make_async_copy(tf_hbm, tf_v, in_sem.at[0])
    ti_in = pltpu.make_async_copy(ti_hbm, ti_v, in_sem.at[1])
    tf_in.start()
    for x in range(n_col):
        f_in(x).start()

    def table_copy(src, dst, sem, k):
        low = k * groups
        return pltpu.make_async_copy(src.at[k * groups + me, pl.ds(low, l_max - low), :], dst.at[k, pl.ds(low, l_max - low), :], sem.at[k])

    n_slot = stage.shape[0]
    w_blk = stage.shape[1] // (2 * n_chan)
    n_blk = l_max // w_blk
    blk_rows = stage.shape[1]

    def w_copy(b, slot):
        return pltpu.make_async_copy(w_hbm.at[pl.ds((n_blk - 1 - b) * blk_rows, blk_rows), :], stage.at[slot], w_sem.at[slot])

    for s in range(n_slot):
        w_copy(s, s).start()
    for k in reversed(range(per_dev)):
        table_copy(pw_hbm, pw_v, pw_sem, k).start()
        low, first = k * groups, (k // piece) * l_step
        if low > first:
            pw_v[k, first:low, :] = jnp.zeros((low - first, n_lat), F32)
            pi_v[k, first:low, :] = jnp.zeros((low - first, n_lat), F32)
        table_copy(pi_hbm, pi_v, pi_sem, k).start()
    ti_in.start()

    tf_in.wait()
    for x in range(n_col):
        f_in(x).wait()

    def dft(u, _):
        out = []
        for half in range(2):
            here = pl.ds(2 * u + half, n_chan, stride=lat_loc)
            f_t = jnp.concatenate([f_v[x, here, :] for x in range(n_col)], axis=1).astype(BF16)
            r = dot(tf_v[...], f_t, ((1,), (1,)))
            out.append(r.reshape(n_chunk * groups, rows, n_chan))
        f_send[:, pl.ds(pl.multiple_of(u * 2 * rows, 2 * rows), 2 * rows), :] = jnp.concatenate(out, axis=1).astype(BF16)
        return 0

    lax.fori_loop(0, lat_loc // 2, dft, 0)
    pl.semaphore_wait(barrier, groups - 1)

    def fwd_copy(j, to, slot):
        return pltpu.make_async_remote_copy(
            src_ref=f_send.at[j * groups + to], dst_ref=f_recv.at[j * groups + slot], send_sem=fs_sem.at[j, to],
            recv_sem=fr_sem.at[j, slot], device_id=(member, to), device_id_type=MESH)

    def back_copy(j, to, slot):
        return pltpu.make_async_remote_copy(
            src_ref=g_send.at[j * groups + to], dst_ref=g_recv.at[j * groups + slot], send_sem=gs_sem.at[j, to],
            recv_sem=gr_sem.at[j, slot], device_id=(member, to), device_id_type=MESH)

    def send_all(copy, src, dst, j, own):
        pltpu.make_async_copy(src.at[j * groups + me], dst.at[j * groups + me], own_sem.at[own]).start()

        def go(i, _):
            copy(j, peer(i), me).start()
            return 0

        lax.fori_loop(0, groups - 1, go, 0)

    def recv_all(copy, src, dst, j, own):
        pltpu.make_async_copy(src.at[j * groups + me], dst.at[j * groups + me], own_sem.at[own]).wait()

        def got(i, _):
            s = lax.rem(me + i, groups)
            copy(j, s, s).wait_recv()
            return 0

        lax.fori_loop(1, groups, got, 0)

    def sent_all(copy, j):
        def done(i, _):
            s = lax.rem(me + i, groups)
            copy(j, s, s).wait_send()
            return 0

        lax.fori_loop(1, groups, done, 0)

    order = list(reversed(range(n_chunk)))
    for j in order:
        send_all(fwd_copy, f_send, f_recv, j, j)

    sign = jnp.where(lax.broadcasted_iota(jnp.int32, (rows, n_chan), 0) < piece, -1.0, 1.0).astype(F32)

    def load_w(b, _):
        slot = lax.rem(b, n_slot)
        w_copy(b, slot).wait()
        half = blk_rows // 2
        re = stage[slot, pl.ds(0, half, stride=2), :]
        im = stage[slot, pl.ds(1, half, stride=2), :]
        at = pl.ds(pl.multiple_of((n_blk - 1 - b) * half, half), half)
        w_v[at, :n_chan] = re.astype(BF16)
        w_v[at, n_chan:] = im.astype(BF16)

        @pl.when(b + n_slot < n_blk)
        def _():
            w_copy(b + n_slot, slot).start()

        return 0

    blk_chunk = n_blk // n_chunk
    n_row = n_lat * rows
    for at, j in enumerate(order):
        lax.fori_loop(at * blk_chunk, (at + 1) * blk_chunk, load_w, 0)
        recv_all(fwd_copy, f_send, f_recv, j, j)
        low = j * l_step
        n_l = l_max - low

        def widen(s, _):
            wide[pl.ds(pl.multiple_of(s * block, block), block), :] = f_recv[j * groups + s].astype(F32)
            return 0

        lax.fori_loop(0, groups, widen, 0)
        for i in range(piece):
            k = j * piece + i
            table_copy(pw_hbm, pw_v, pw_sem, k).wait()
            re = wide[pl.ds(i, n_lat, stride=rows), :]
            im = wide[pl.ds(piece + i, n_lat, stride=rows), :]
            spec = jnp.concatenate([re, im], axis=1).astype(BF16)
            a = dot(pw_v[k, low:, :].astype(BF16), spec, ((1,), (0,)))
            coef[pl.ds(low * rows + i, n_l, stride=rows), :] = a[:, :n_chan]
            coef[pl.ds(low * rows + piece + i, n_l, stride=rows), :] = a[:, n_chan:]

        def mix(v, _):
            for e in range(8):
                deg = v * 8 + e
                here = pl.ds(pl.multiple_of(deg * rows, rows), rows)
                w_l = w_v[pl.ds(pl.multiple_of(deg * n_chan, n_chan), n_chan), :]
                r = dot(coef[here, :].astype(BF16), w_l, ((1,), (0,)))
                coef[here, :] = r[:, :n_chan] + sign * pltpu.roll(r[:, n_chan:], piece, 0)
            return 0

        lax.fori_loop(low // 8, l_max // 8, mix, 0)
        for i in range(piece):
            k = j * piece + i
            table_copy(pi_hbm, pi_v, pi_sem, k).wait()
            re = coef[pl.ds(low * rows + i, n_l, stride=rows), :]
            im = coef[pl.ds(low * rows + piece + i, n_l, stride=rows), :]
            b = jnp.concatenate([re, im], axis=1).astype(BF16)
            g = dot(pi_v[k, low:, :].astype(BF16), b, ((0,), (0,)))
            wide[pl.ds(i, n_lat, stride=rows), :] = g[:, :n_chan]
            wide[pl.ds(piece + i, n_lat, stride=rows), :] = g[:, n_chan:]

        def narrow(s, _):
            g_send[j * groups + s] = wide[pl.ds(pl.multiple_of(s * block, block), block), :].astype(BF16)
            return 0

        lax.fori_loop(0, groups, narrow, 0)
        send_all(back_copy, g_send, g_recv, j, n_chunk + j)

    ti_in.wait()
    for at, j in enumerate(order):
        recv_all(back_copy, g_send, g_recv, j, n_chunk + j)
        last = at == n_chunk - 1

        def inverse(u, _):
            pair = g_recv[j * groups:(j + 1) * groups, pl.ds(pl.multiple_of(u * 2 * rows, 2 * rows), 2 * rows), :].astype(F32)
            for half in range(2):
                t = 2 * u + half
                g_t = pair[:, half * rows:(half + 1) * rows, :].reshape(groups * rows, n_chan)
                h = dot(g_t.T.astype(BF16), ti_v[j * groups * rows:(j + 1) * groups * rows, :], ((1,), (0,)))
                if at > 0:
                    h = h + h_v[t]
                if last:
                    here = pl.ds(t, n_chan, stride=lat_loc)
                    g = jax.nn.gelu(h)
                    for x in range(n_col):
                        f_v[x, here, :] = f_v[x, here, :] + g[:, x * LANES:(x + 1) * LANES]
                else:
                    h_v[t] = h
            return 0

        lax.fori_loop(0, lat_loc // 2, inverse, 0)
    for x in range(n_col):
        f_out(x).start()
    for j in order:
        sent_all(fwd_copy, j)
        sent_all(back_copy, j)
    for x in range(n_col):
        f_out(x).wait()


def solution(mesh):
    groups = mesh.shape["lat"]

    def local_layer(field_loc, p_fwd, p_inv, w_mix):
        n_chan, lat_loc, n_lon = field_loc.shape
        l_max, _, n_lat = p_fwd.shape
        per_dev = l_max // groups
        rows = 2 * per_dev // N_CHUNK
        block = lat_loc * rows
        fwd_tab, inv_tab = wave_tables(n_lon, groups, per_dev, N_CHUNK)
        w_rows = w_mix.transpose(0, 1, 3, 2).reshape(l_max * n_chan * 2, n_chan)
        hbm = pl.BlockSpec(memory_space=pltpu.HBM)
        exchange = pltpu.VMEM((N_CHUNK * groups, block, n_chan), BF16)
        dma = pltpu.SemaphoreType.DMA
        out = pl.pallas_call(
            functools.partial(layer_kernel, (groups, n_chan, lat_loc, n_lon, l_max, n_lat, N_CHUNK)),
            out_shape=jax.ShapeDtypeStruct((n_chan * lat_loc, n_lon), F32),
            in_specs=[hbm] * 6,
            out_specs=hbm,
            scratch_shapes=[
                pltpu.VMEM((n_lon // LANES, n_chan * lat_loc, LANES), F32),
                pltpu.VMEM((lat_loc, n_chan, n_lon), F32),
                pltpu.VMEM((l_max * n_chan, 2 * n_chan), BF16),
                pltpu.VMEM((4, 8 * n_chan * 2, n_chan), F32),
                pltpu.VMEM((per_dev, l_max, n_lat), F32),
                pltpu.VMEM((per_dev, l_max, n_lat), F32),
                exchange, exchange, exchange, exchange,
                pltpu.VMEM((n_lat * rows, n_chan), F32),
                pltpu.VMEM((l_max * rows, n_chan), F32),
                pltpu.VMEM(fwd_tab.shape, BF16),
                pltpu.VMEM(inv_tab.shape, BF16),
                dma((2,)), dma((n_lon // LANES,)), dma((per_dev,)), dma((per_dev,)), dma((4,)), dma((2 * N_CHUNK,)),
                dma((N_CHUNK, groups)), dma((N_CHUNK, groups)), dma((N_CHUNK, groups)), dma((N_CHUNK, groups)),
            ],
            compiler_params=pltpu.CompilerParams(collective_id=0, has_side_effects=True, vmem_limit_bytes=62 * 2**20),
            name="spectral_layer",
        )(field_loc.reshape(n_chan * lat_loc, n_lon), p_fwd, p_inv, w_rows, fwd_tab, inv_tab)
        return out.reshape(field_loc.shape)

    return jax.shard_map(local_layer, mesh=mesh, in_specs=(P("member", "lat", None), P(), P(), P()), out_specs=P("member", "lat", None), check_vma=False)
```

```python
import functools
import math

import jax
import jax.numpy as jnp
import numpy as np
from jax import lax
from jax.experimental import pallas as pl
from jax.experimental.pallas import tpu as pltpu
from jax.sharding import PartitionSpec as P

MESH = pl.DeviceIdType.MESH
F32 = jnp.float32
BF16 = jnp.bfloat16
LANES = 128
N_CHUNK = 4


def wave_tables(n_lon, groups, per_dev, n_chunk):
    piece = per_dev // n_chunk
    chunk, dev, part, k = np.meshgrid(np.arange(n_chunk), np.arange(groups), np.arange(2), np.arange(piece), indexing="ij")
    wave = ((chunk * piece + k) * groups + dev).reshape(-1, 1)
    part = part.reshape(-1, 1)
    angle = ((wave * np.arange(n_lon)[None, :]) % n_lon) * (2.0 * math.pi / n_lon)
    fwd = np.where(part == 0, np.cos(angle), -np.sin(angle)).astype(np.float32)
    inv = fwd * np.where(wave == 0, 1.0, 2.0).astype(np.float32)
    return jnp.asarray(fwd, BF16), jnp.asarray(inv, BF16)


def dot(a, b, dims):
    return lax.dot_general(a, b, (dims, ((), ())), preferred_element_type=F32)


def layer_kernel(dims, f_hbm, pw_hbm, pi_hbm, w_hbm, tf_hbm, ti_hbm, *refs):
    n_out = dims[3] // LANES
    o_v, refs = refs[:n_out], refs[n_out:]
    (f_v, f_b, h_v, w_v, stage, pw_v, pi_v, f_send, f_recv, g_send, g_recv, wide, coef, tf_v, ti_v,
                 in_sem, f_sem, pw_sem, pi_sem, w_sem, own_sem, fs_sem, fr_sem, gs_sem, gr_sem) = refs
    groups, n_chan, lat_loc, n_lon, l_max, n_lat, n_chunk = dims
    per_dev = l_max // groups
    piece = per_dev // n_chunk
    rows = 2 * piece
    block = lat_loc * rows
    l_step = l_max // n_chunk
    member, me = lax.axis_index("member"), lax.axis_index("lat")
    n_z = groups // 2
    z, core = me // 2, lax.rem(me, 2)

    def peer(i):
        step = i // 2
        dist = n_z // 2 - (step + 1) // 2
        dz = jnp.where(lax.rem(step, 2) == 1, dist, -dist)
        far = lax.rem(z + dz + n_z, n_z) * 2 + lax.rem(i, 2)
        return jnp.where(i == groups - 2, z * 2 + 1 - core, far)

    barrier = pltpu.get_barrier_semaphore()

    def greet(i, _):
        pl.semaphore_signal(barrier, inc=1, device_id=(member, peer(i)), device_id_type=MESH)
        return 0

    lax.fori_loop(0, groups - 1, greet, 0)

    n_col = n_lon // LANES

    half = lat_loc // 2

    def f_in(h, x):
        part = pl.ds(h * half, half)
        return pltpu.make_async_copy(f_hbm.at[:, part, pl.ds(x * LANES, LANES)], f_v.at[x, :, part, :], f_sem.at[h, x])

    tf_in = pltpu.make_async_copy(tf_hbm, tf_v, in_sem.at[0])
    ti_in = pltpu.make_async_copy(ti_hbm, ti_v, in_sem.at[1])
    tf_in.start()
    for h in range(2):
        for x in range(n_col):
            f_in(h, x).start()

    def table_copy(src, dst, sem, k):
        low = k * groups
        return pltpu.make_async_copy(src.at[k * groups + me, pl.ds(low, l_max - low), :], dst.at[k, pl.ds(low, l_max - low), :], sem.at[k])

    n_slot = stage.shape[0]
    w_blk = stage.shape[1] // (2 * n_chan)
    n_blk = l_max // w_blk
    blk_rows = stage.shape[1]

    def w_copy(b, slot):
        return pltpu.make_async_copy(w_hbm.at[pl.ds((n_blk - 1 - b) * blk_rows, blk_rows), :], stage.at[slot], w_sem.at[slot])

    def start_loads():
        for s in range(n_slot):
            w_copy(s, s).start()
        for k in reversed(range(per_dev)):
            table_copy(pw_hbm, pw_v, pw_sem, k).start()
            low, first = k * groups, (k // piece) * l_step
            if low > first:
                pw_v[k, first:low, :] = jnp.zeros((low - first, n_lat), F32)
                pi_v[k, first:low, :] = jnp.zeros((low - first, n_lat), F32)
            table_copy(pi_hbm, pi_v, pi_sem, k).start()
        ti_in.start()

    tf_in.wait()
    f_rows = f_v.reshape(n_col, n_chan * lat_loc, LANES)

    def dft_out(j, u, f_pair):
        r = dot(tf_v[j * groups * rows:(j + 1) * groups * rows, :], f_pair, ((1,), (1,)))
        both = [r[:, e * n_chan:(e + 1) * n_chan].reshape(groups, rows, n_chan) for e in range(2)]
        at = pl.ds(pl.multiple_of(u * 2 * rows, 2 * rows), 2 * rows)
        f_send[j * groups:(j + 1) * groups, at, :] = jnp.concatenate(both, axis=1).astype(BF16)

    def dft_first(u, _):
        pair = []
        for e in range(2):
            here = pl.ds(2 * u + e, n_chan, stride=lat_loc)
            pair.append(jnp.concatenate([f_rows[x, here, :] for x in range(n_col)], axis=1))
        f_pair = jnp.concatenate(pair, axis=0).astype(BF16)
        f_b[u] = f_pair
        dft_out(n_chunk - 1, u, f_pair)
        return 0

    for h in range(2):
        for x in range(n_col):
            f_in(h, x).wait()
        if h == 1:
            start_loads()
        lax.fori_loop(h * half // 2, (h + 1) * half // 2, dft_first, 0)
    pl.semaphore_wait(barrier, groups - 1)

    def fwd_copy(j, to, slot):
        return pltpu.make_async_remote_copy(
            src_ref=f_send.at[j * groups + to], dst_ref=f_recv.at[j * groups + slot], send_sem=fs_sem.at[j, to],
            recv_sem=fr_sem.at[j, slot], device_id=(member, to), device_id_type=MESH)

    def back_copy(p, to, slot):
        j, part = (p, pl.ds(0, block)) if p else (0, pl.ds(0, block // 2))
        if p == n_chunk:
            j, part = 0, pl.ds(block // 2, block // 2)
        return pltpu.make_async_remote_copy(
            src_ref=g_send.at[j * groups + to, part], dst_ref=g_recv.at[j * groups + slot, part], send_sem=gs_sem.at[p, to],
            recv_sem=gr_sem.at[p, slot], device_id=(member, to), device_id_type=MESH)

    def own_copy(src, dst, j, own):
        return pltpu.make_async_copy(src.at[j * groups + me], dst.at[j * groups + me], own_sem.at[own])

    def send_all(copy, j):
        def go(i, _):
            copy(j, peer(i), me).start()
            return 0

        lax.fori_loop(0, groups - 1, go, 0)

    def recv_all(copy, j):
        def got(i, _):
            s = lax.rem(me + i, groups)
            copy(j, s, s).wait_recv()
            return 0

        lax.fori_loop(1, groups, got, 0)

    def sent_all(copy, j):
        def done(i, _):
            s = lax.rem(me + i, groups)
            copy(j, s, s).wait_send()
            return 0

        lax.fori_loop(1, groups, done, 0)

    order = list(reversed(range(n_chunk)))
    for j in order:
        if j < n_chunk - 1:
            lax.fori_loop(0, lat_loc // 2, lambda u, _, j=j: dft_out(j, u, f_b[u]) or 0, 0)
        own_copy(f_send, f_recv, j, j).start()
        send_all(fwd_copy, j)

    sign = jnp.where(lax.broadcasted_iota(jnp.int32, (rows, n_chan), 0) < piece, -1.0, 1.0).astype(F32)

    def load_w(b, _):
        slot = lax.rem(b, n_slot)
        w_copy(b, slot).wait()
        half = blk_rows // 2
        re = stage[slot, pl.ds(0, half, stride=2), :]
        im = stage[slot, pl.ds(1, half, stride=2), :]
        at = pl.ds(pl.multiple_of((n_blk - 1 - b) * half, half), half)
        w_v[at, :n_chan] = re.astype(BF16)
        w_v[at, n_chan:] = im.astype(BF16)

        @pl.when(b + n_slot < n_blk)
        def _():
            w_copy(b + n_slot, slot).start()

        return 0

    blk_chunk = n_blk // n_chunk
    n_row = n_lat * rows
    for at, j in enumerate(order):
        lax.fori_loop(at * blk_chunk, (at + 1) * blk_chunk, load_w, 0)
        own_copy(f_send, f_recv, j, j).wait()
        recv_all(fwd_copy, j)
        low = j * l_step
        n_l = l_max - low

        def widen(s, _):
            wide[pl.ds(pl.multiple_of(s * block, block), block), :] = f_recv[j * groups + s].astype(F32)
            return 0

        lax.fori_loop(0, groups, widen, 0)
        for i in range(piece):
            k = j * piece + i
            table_copy(pw_hbm, pw_v, pw_sem, k).wait()
            re = wide[pl.ds(i, n_lat, stride=rows), :]
            im = wide[pl.ds(piece + i, n_lat, stride=rows), :]
            spec = jnp.concatenate([re, im], axis=1).astype(BF16)
            a = dot(pw_v[k, low:, :].astype(BF16), spec, ((1,), (0,)))
            coef[pl.ds(low * rows + i, n_l, stride=rows), :] = a[:, :n_chan]
            coef[pl.ds(low * rows + piece + i, n_l, stride=rows), :] = a[:, n_chan:]

        def mix(v, _):
            for e in range(8):
                deg = v * 8 + e
                here = pl.ds(pl.multiple_of(deg * rows, rows), rows)
                w_l = w_v[pl.ds(pl.multiple_of(deg * n_chan, n_chan), n_chan), :]
                r = dot(coef[here, :].astype(BF16), w_l, ((1,), (0,)))
                coef[here, :] = r[:, :n_chan] + sign * pltpu.roll(r[:, n_chan:], piece, 0)
            return 0

        lax.fori_loop(low // 8, l_max // 8, mix, 0)
        for i in range(piece):
            k = j * piece + i
            table_copy(pi_hbm, pi_v, pi_sem, k).wait()
            re = coef[pl.ds(low * rows + i, n_l, stride=rows), :]
            im = coef[pl.ds(low * rows + piece + i, n_l, stride=rows), :]
            b = jnp.concatenate([re, im], axis=1).astype(BF16)
            g = dot(pi_v[k, low:, :].astype(BF16), b, ((0,), (0,)))
            wide[pl.ds(i, n_lat, stride=rows), :] = g[:, :n_chan]
            wide[pl.ds(piece + i, n_lat, stride=rows), :] = g[:, n_chan:]

        def narrow(s, _):
            g_send[j * groups + s] = wide[pl.ds(pl.multiple_of(s * block, block), block), :].astype(BF16)
            return 0

        lax.fori_loop(0, groups, narrow, 0)
        own_copy(g_send, g_recv, j, n_chunk + j).start()
        send_all(back_copy, j)
        if j == 0:
            send_all(back_copy, n_chunk)

    ti_in.wait()
    for at, j in enumerate(order):
        own_copy(g_send, g_recv, j, n_chunk + j).wait()
        recv_all(back_copy, j)
        last = at == n_chunk - 1

        def inverse(u, _):
            pair = g_recv[j * groups:(j + 1) * groups, pl.ds(pl.multiple_of(u * 2 * rows, 2 * rows), 2 * rows), :].astype(F32)
            for half in range(2):
                t = 2 * u + half
                g_t = pair[:, half * rows:(half + 1) * rows, :].reshape(groups * rows, n_chan)
                h = dot(g_t.T.astype(BF16), ti_v[j * groups * rows:(j + 1) * groups * rows, :], ((1,), (0,)))
                if at > 0:
                    h = h + h_v[t]
                if last:
                    here = pl.ds(t, n_chan, stride=lat_loc)
                    g = jax.nn.gelu(h)
                    for x in range(n_col):
                        o_v[x][here, :] = f_rows[x, here, :] + g[:, x * LANES:(x + 1) * LANES]
                else:
                    h_v[t] = h
            return 0

        if last:
            lax.fori_loop(0, lat_loc // 4, inverse, 0)
            recv_all(back_copy, n_chunk)
            lax.fori_loop(lat_loc // 4, lat_loc // 2, inverse, 0)
        else:
            lax.fori_loop(0, lat_loc // 2, inverse, 0)
    for j in order:
        sent_all(fwd_copy, j)
        sent_all(back_copy, j)
    sent_all(back_copy, n_chunk)


def solution(mesh):
    groups = mesh.shape["lat"]

    def local_layer(field_loc, p_fwd, p_inv, w_mix):
        n_chan, lat_loc, n_lon = field_loc.shape
        l_max, _, n_lat = p_fwd.shape
        per_dev = l_max // groups
        rows = 2 * per_dev // N_CHUNK
        block = lat_loc * rows
        fwd_tab, inv_tab = wave_tables(n_lon, groups, per_dev, N_CHUNK)
        w_rows = w_mix.transpose(0, 1, 3, 2).reshape(l_max * n_chan * 2, n_chan)
        hbm = pl.BlockSpec(memory_space=pltpu.HBM)
        exchange = pltpu.VMEM((N_CHUNK * groups, block, n_chan), BF16)
        dma = pltpu.SemaphoreType.DMA
        out = pl.pallas_call(
            functools.partial(layer_kernel, (groups, n_chan, lat_loc, n_lon, l_max, n_lat, N_CHUNK)),
            out_shape=[pltpu.VMEM((n_chan * lat_loc, LANES), F32)] * (n_lon // LANES),
            in_specs=[hbm] * 6,
            out_specs=[pl.BlockSpec(memory_space=pltpu.VMEM)] * (n_lon // LANES),
            scratch_shapes=[
                pltpu.VMEM((n_lon // LANES, n_chan, lat_loc, LANES), F32),
                pltpu.VMEM((lat_loc // 2, 2 * n_chan, n_lon), BF16),
                pltpu.VMEM((lat_loc, n_chan, n_lon), F32),
                pltpu.VMEM((l_max * n_chan, 2 * n_chan), BF16),
                pltpu.VMEM((4, 8 * n_chan * 2, n_chan), F32),
                pltpu.VMEM((per_dev, l_max, n_lat), F32),
                pltpu.VMEM((per_dev, l_max, n_lat), F32),
                exchange, exchange, exchange, exchange,
                pltpu.VMEM((n_lat * rows, n_chan), F32),
                pltpu.VMEM((l_max * rows, n_chan), F32),
                pltpu.VMEM(fwd_tab.shape, BF16),
                pltpu.VMEM(inv_tab.shape, BF16),
                dma((2,)), dma((2, n_lon // LANES)), dma((per_dev,)), dma((per_dev,)), dma((4,)), dma((2 * N_CHUNK,)),
                dma((N_CHUNK, groups)), dma((N_CHUNK, groups)), dma((N_CHUNK + 1, groups)), dma((N_CHUNK + 1, groups)),
            ],
            compiler_params=pltpu.CompilerParams(collective_id=0, has_side_effects=True, vmem_limit_bytes=54 * 2**20),
            name="spectral_layer",
        )(field_loc, p_fwd, p_inv, w_rows, fwd_tab, inv_tab)
        return jnp.concatenate([part.reshape(n_chan, lat_loc, LANES) for part in out], axis=2)

    return jax.shard_map(local_layer, mesh=mesh, in_specs=(P("member", "lat", None), P(), P(), P()), out_specs=P("member", "lat", None), check_vma=False)
```

```python
import functools
import math

import jax
import jax.numpy as jnp
import numpy as np
from jax import lax
from jax.experimental import pallas as pl
from jax.experimental.pallas import tpu as pltpu
from jax.sharding import PartitionSpec as P

MESH = pl.DeviceIdType.MESH
F32 = jnp.float32
BF16 = jnp.bfloat16
LANES = 128
N_CHUNK = 4


def wave_tables(n_lon, groups, per_dev, n_chunk):
    piece = per_dev // n_chunk
    chunk, dev, part, k = np.meshgrid(np.arange(n_chunk), np.arange(groups), np.arange(2), np.arange(piece), indexing="ij")
    wave = ((chunk * piece + k) * groups + dev).reshape(-1, 1)
    part = part.reshape(-1, 1)
    angle = ((wave * np.arange(n_lon)[None, :]) % n_lon) * (2.0 * math.pi / n_lon)
    fwd = np.where(part == 0, np.cos(angle), -np.sin(angle)).astype(np.float32)
    inv = fwd * np.where(wave == 0, 1.0, 2.0).astype(np.float32)
    return jnp.asarray(fwd, BF16), jnp.asarray(inv, BF16)


def dot(a, b, dims):
    return lax.dot_general(a, b, (dims, ((), ())), preferred_element_type=F32)


def layer_kernel(dims, f_hbm, pw_hbm, pi_hbm, w_hbm, tf_hbm, ti_hbm, *refs):
    n_out = dims[3] // LANES
    o_v, refs = refs[:n_out], refs[n_out:]
    (f_v, f_b, h_v, w_v, stage, pw_v, pi_v, f_send, f_recv, g_send, g_recv, wide, coef, b_all, pi_loc, tf_v, ti_v,
                 in_sem, f_sem, pw_sem, pi_sem, w_sem, own_sem, fs_sem, fr_sem, gs_sem, gr_sem, hop_s, hop_r, sib_s, sib_r) = refs
    groups, n_chan, lat_loc, n_lon, l_max, n_lat, n_chunk = dims
    per_dev = l_max // groups
    piece = per_dev // n_chunk
    rows = 2 * piece
    block = lat_loc * rows
    l_step = l_max // n_chunk
    top = n_chunk - 1
    heights = [l_max - (top * piece + i) * groups for i in range(piece)]
    starts = [sum(heights[:i]) for i in range(piece)]
    b_rows = sum(heights)
    member, me = lax.axis_index("member"), lax.axis_index("lat")
    n_z = groups // 2
    z, core = me // 2, lax.rem(me, 2)

    def peer(i):
        step = i // 2
        dist = n_z // 2 - (step + 1) // 2
        dz = jnp.where(lax.rem(step, 2) == 1, dist, -dist)
        far = lax.rem(z + dz + n_z, n_z) * 2 + lax.rem(i, 2)
        return jnp.where(i == groups - 2, z * 2 + 1 - core, far)

    barrier = pltpu.get_barrier_semaphore()

    def greet(i, _):
        pl.semaphore_signal(barrier, inc=1, device_id=(member, peer(i)), device_id_type=MESH)
        return 0

    lax.fori_loop(0, groups - 1, greet, 0)

    n_col = n_lon // LANES

    half = lat_loc // 2

    def f_in(h, x):
        part = pl.ds(h * half, half)
        return pltpu.make_async_copy(f_hbm.at[:, part, pl.ds(x * LANES, LANES)], f_v.at[x, :, part, :], f_sem.at[h, x])

    tf_in = pltpu.make_async_copy(tf_hbm, tf_v, in_sem.at[0])
    ti_in = pltpu.make_async_copy(ti_hbm, ti_v, in_sem.at[1])
    tf_in.start()
    for h in range(2):
        for x in range(n_col):
            f_in(h, x).start()

    def table_copy(src, dst, sem, k):
        low = k * groups
        return pltpu.make_async_copy(src.at[k * groups + me, pl.ds(low, l_max - low), :], dst.at[k, pl.ds(low, l_max - low), :], sem.at[k])

    n_slot = stage.shape[0]
    w_blk = stage.shape[1] // (2 * n_chan)
    n_blk = l_max // w_blk
    blk_rows = stage.shape[1]

    def w_copy(b, slot):
        return pltpu.make_async_copy(w_hbm.at[pl.ds((n_blk - 1 - b) * blk_rows, blk_rows), :], stage.at[slot], w_sem.at[slot])

    lane = me * lat_loc // LANES * LANES
    pi_loc_in = pltpu.make_async_copy(
        pi_hbm.at[pl.ds(top * piece * groups, piece * groups), pl.ds(top * l_step, l_step), pl.ds(pl.multiple_of(lane, LANES), LANES)],
        pi_loc, in_sem.at[2])

    def start_loads():
        for s in range(n_slot):
            w_copy(s, s).start()
        for k in reversed(range(per_dev)):
            table_copy(pw_hbm, pw_v, pw_sem, k).start()
            if k < top * piece:
                table_copy(pi_hbm, pi_v, pi_sem, k).start()
            low, first = k * groups, (k // piece) * l_step
            if low > first:
                pw_v[k, first:low, :] = jnp.zeros((low - first, n_lat), F32)
                if k < top * piece:
                    pi_v[k, first:low, :] = jnp.zeros((low - first, n_lat), F32)
        pi_loc_in.start()
        ti_in.start()

    tf_in.wait()
    f_rows = f_v.reshape(n_col, n_chan * lat_loc, LANES)

    def dft_out(j, u, f_pair):
        r = dot(tf_v[j * groups * rows:(j + 1) * groups * rows, :], f_pair, ((1,), (1,)))
        both = [r[:, e * n_chan:(e + 1) * n_chan].reshape(groups, rows, n_chan) for e in range(2)]
        at = pl.ds(pl.multiple_of(u * 2 * rows, 2 * rows), 2 * rows)
        f_send[j * groups:(j + 1) * groups, at, :] = jnp.concatenate(both, axis=1).astype(BF16)

    def dft_first(u, _):
        pair = []
        for e in range(2):
            here = pl.ds(2 * u + e, n_chan, stride=lat_loc)
            pair.append(jnp.concatenate([f_rows[x, here, :] for x in range(n_col)], axis=1))
        f_pair = jnp.concatenate(pair, axis=0).astype(BF16)
        f_b[u] = f_pair
        dft_out(n_chunk - 1, u, f_pair)
        return 0

    for h in range(2):
        for x in range(n_col):
            f_in(h, x).wait()
        if h == 1:
            start_loads()
        lax.fori_loop(h * half // 2, (h + 1) * half // 2, dft_first, 0)
    pl.semaphore_wait(barrier, groups - 1)

    def fwd_copy(j, to, slot):
        return pltpu.make_async_remote_copy(
            src_ref=f_send.at[j * groups + to], dst_ref=f_recv.at[j * groups + slot], send_sem=fs_sem.at[j, to],
            recv_sem=fr_sem.at[j, slot], device_id=(member, to), device_id_type=MESH)

    def back_copy(p, to, slot):
        j, part = (p, pl.ds(0, block)) if p else (0, pl.ds(0, block // 2))
        if p == n_chunk:
            j, part = 0, pl.ds(block // 2, block // 2)
        return pltpu.make_async_remote_copy(
            src_ref=g_send.at[j * groups + to, part], dst_ref=g_recv.at[j * groups + slot, part], send_sem=gs_sem.at[p, to],
            recv_sem=gr_sem.at[p, slot], device_id=(member, to), device_id_type=MESH)

    def own_copy(src, dst, j, own):
        return pltpu.make_async_copy(src.at[j * groups + me], dst.at[j * groups + me], own_sem.at[own])

    def send_all(copy, j):
        def go(i, _):
            copy(j, peer(i), me).start()
            return 0

        lax.fori_loop(0, groups - 1, go, 0)

    def recv_all(copy, j):
        def got(i, _):
            s = lax.rem(me + i, groups)
            copy(j, s, s).wait_recv()
            return 0

        lax.fori_loop(1, groups, got, 0)

    def sent_all(copy, j):
        def done(i, _):
            s = lax.rem(me + i, groups)
            copy(j, s, s).wait_send()
            return 0

        lax.fori_loop(1, groups, done, 0)

    n_hop = n_z // 2

    def b_part(h, sgn):
        if h < n_hop:
            return pl.ds(0, b_rows)
        return pl.ds(0 if sgn > 0 else b_rows // 2, b_rows // 2)

    def chip(dz):
        return lax.rem(z + dz + n_z, n_z)

    def b_remote(s, part, to, sems, n):
        return pltpu.make_async_remote_copy(
            src_ref=b_all.at[s, part], dst_ref=b_all.at[s, part], send_sem=sems[0].at[n], recv_sem=sems[1].at[n],
            device_id=(member, to), device_id_type=MESH)

    def hop(h, sgn, arriving):
        s = chip(-sgn * (h if arriving else h - 1)) * 2 + core
        n = (h - 1) * 2 + (sgn < 0)
        return b_remote(s, b_part(h, sgn), chip(sgn) * 2 + core, (hop_s, hop_r), n)

    def sib(h, sgn, arriving):
        s = chip(-sgn * h) * 2 + (1 - core if arriving else core)
        n = 0 if h == 0 else (h - 1) * 2 + (sgn < 0) + 1
        return b_remote(s, b_part(h, sgn), z * 2 + 1 - core, (sib_s, sib_r), n)

    hops = [(h, sgn) for h in range(1, n_hop + 1) for sgn in (1, -1)]

    def relay(h):
        for sgn in (1, -1):
            if h > 0:
                hop(h, sgn, True).wait_recv()
            if h < n_hop:
                hop(h + 1, sgn, False).start()
            if h > 0 or sgn > 0:
                sib(h, sgn, False).start()

    def b_done():
        for h, sgn in hops:
            hop(h, sgn, False).wait_send()
        for h, sgn in [(0, 1)] + hops:
            sib(h, sgn, False).wait_send()

    order = list(reversed(range(n_chunk)))

    def send_fwd(j):
        own_copy(f_send, f_recv, j, j).start()
        send_all(fwd_copy, j)

    def send_back(j):
        own_copy(g_send, g_recv, j, n_chunk + j).start()
        send_all(back_copy, j)
        if j == 0:
            send_all(back_copy, n_chunk)

    send_fwd(top)
    for j in order[1:]:
        lax.fori_loop(0, lat_loc // 2, lambda u, _, j=j: dft_out(j, u, f_b[u]) or 0, 0)
        if j == top - 1:
            send_fwd(j)

    sign = jnp.where(lax.broadcasted_iota(jnp.int32, (rows, n_chan), 0) < piece, -1.0, 1.0).astype(F32)

    def load_w(b, _):
        slot = lax.rem(b, n_slot)
        w_copy(b, slot).wait()
        half = blk_rows // 2
        re = stage[slot, pl.ds(0, half, stride=2), :]
        im = stage[slot, pl.ds(1, half, stride=2), :]
        at = pl.ds(pl.multiple_of((n_blk - 1 - b) * half, half), half)
        w_v[at, :n_chan] = re.astype(BF16)
        w_v[at, n_chan:] = im.astype(BF16)

        @pl.when(b + n_slot < n_blk)
        def _():
            w_copy(b + n_slot, slot).start()

        return 0

    blk_chunk = n_blk // n_chunk
    n_row = n_lat * rows
    for at, j in enumerate(order):
        lax.fori_loop(at * blk_chunk, (at + 1) * blk_chunk, load_w, 0)
        own_copy(f_send, f_recv, j, j).wait()
        recv_all(fwd_copy, j)
        low = j * l_step
        n_l = l_max - low

        def widen(s, _):
            wide[pl.ds(pl.multiple_of(s * block, block), block), :] = f_recv[j * groups + s].astype(F32)
            return 0

        lax.fori_loop(0, groups, widen, 0)
        for i in range(piece):
            k = j * piece + i
            table_copy(pw_hbm, pw_v, pw_sem, k).wait()
            re = wide[pl.ds(i, n_lat, stride=rows), :]
            im = wide[pl.ds(piece + i, n_lat, stride=rows), :]
            spec = jnp.concatenate([re, im], axis=1).astype(BF16)
            a = dot(pw_v[k, low:, :].astype(BF16), spec, ((1,), (0,)))
            coef[pl.ds(low * rows + i, n_l, stride=rows), :] = a[:, :n_chan]
            coef[pl.ds(low * rows + piece + i, n_l, stride=rows), :] = a[:, n_chan:]

        def mix(v, _):
            for e in range(8):
                deg = v * 8 + e
                here = pl.ds(pl.multiple_of(deg * rows, rows), rows)
                w_l = w_v[pl.ds(pl.multiple_of(deg * n_chan, n_chan), n_chan), :]
                r = dot(coef[here, :].astype(BF16), w_l, ((1,), (0,)))
                coef[here, :] = r[:, :n_chan] + sign * pltpu.roll(r[:, n_chan:], piece, 0)
            return 0

        lax.fori_loop(low // 8, l_max // 8, mix, 0)
        if j == top:
            for i in range(piece):
                n_i = heights[i]
                base = (l_max - n_i) * rows
                re = coef[pl.ds(base + i, n_i, stride=rows), :]
                im = coef[pl.ds(base + piece + i, n_i, stride=rows), :]
                b_all[me, starts[i]:starts[i] + n_i, :] = jnp.concatenate([re, im], axis=1).astype(BF16)
            relay(0)
            send_fwd(top - 2)
            continue
        for i in range(piece):
            k = j * piece + i
            table_copy(pi_hbm, pi_v, pi_sem, k).wait()
            re = coef[pl.ds(low * rows + i, n_l, stride=rows), :]
            im = coef[pl.ds(low * rows + piece + i, n_l, stride=rows), :]
            b = jnp.concatenate([re, im], axis=1).astype(BF16)
            g = dot(pi_v[k, low:, :].astype(BF16), b, ((0,), (0,)))
            wide[pl.ds(i, n_lat, stride=rows), :] = g[:, :n_chan]
            wide[pl.ds(piece + i, n_lat, stride=rows), :] = g[:, n_chan:]

        def narrow(s, _):
            g_send[j * groups + s] = wide[pl.ds(pl.multiple_of(s * block, block), block), :].astype(BF16)
            return 0

        lax.fori_loop(0, groups, narrow, 0)
        relay(top - j)
        if j == top - 1:
            send_fwd(0)
        if j == top - 2:
            send_back(top - 1)
        if j == 0:
            send_back(1)
            send_back(0)

    def own_rows(d, _):
        for i in range(piece):
            n_i = heights[i]
            p_i = pltpu.roll(pi_loc[i * groups + d, l_step - n_i:, :], lax.rem(lane + LANES - me * lat_loc, LANES), 1)
            g = dot(p_i.T[:lat_loc].astype(BF16), b_all[d, starts[i]:starts[i] + n_i, :], ((1,), (0,)))
            wide[pl.ds(d * block + i, lat_loc, stride=rows), :] = g[:, :n_chan]
            wide[pl.ds(d * block + piece + i, lat_loc, stride=rows), :] = g[:, n_chan:]
        g_recv[top * groups + d] = wide[pl.ds(pl.multiple_of(d * block, block), block), :].astype(BF16)
        return 0

    ti_in.wait()
    back_order = [top - 1, top] + order[2:]
    for at, j in enumerate(back_order):
        if j == top:
            relay(n_hop)
            for h, sgn in [(0, 1)] + hops:
                sib(h, sgn, True).wait_recv()
            pi_loc_in.wait()
            lax.fori_loop(0, groups, own_rows, 0)
        else:
            own_copy(g_send, g_recv, j, n_chunk + j).wait()
            recv_all(back_copy, j)
        last = at == n_chunk - 1

        def inverse(u, _):
            pair = g_recv[j * groups:(j + 1) * groups, pl.ds(pl.multiple_of(u * 2 * rows, 2 * rows), 2 * rows), :].astype(F32)
            for half in range(2):
                t = 2 * u + half
                g_t = pair[:, half * rows:(half + 1) * rows, :].reshape(groups * rows, n_chan)
                h = dot(g_t.T.astype(BF16), ti_v[j * groups * rows:(j + 1) * groups * rows, :], ((1,), (0,)))
                if at > 0:
                    h = h + h_v[t]
                if last:
                    here = pl.ds(t, n_chan, stride=lat_loc)
                    g = jax.nn.gelu(h)
                    for x in range(n_col):
                        o_v[x][here, :] = f_rows[x, here, :] + g[:, x * LANES:(x + 1) * LANES]
                else:
                    h_v[t] = h
            return 0

        if last:
            lax.fori_loop(0, lat_loc // 4, inverse, 0)
            recv_all(back_copy, n_chunk)
            lax.fori_loop(lat_loc // 4, lat_loc // 2, inverse, 0)
        else:
            lax.fori_loop(0, lat_loc // 2, inverse, 0)
    for j in order:
        sent_all(fwd_copy, j)
        if j < top:
            sent_all(back_copy, j)
    b_done()
    sent_all(back_copy, n_chunk)


def solution(mesh):
    groups = mesh.shape["lat"]

    def local_layer(field_loc, p_fwd, p_inv, w_mix):
        n_chan, lat_loc, n_lon = field_loc.shape
        l_max, _, n_lat = p_fwd.shape
        per_dev = l_max // groups
        rows = 2 * per_dev // N_CHUNK
        block = lat_loc * rows
        b_rows = sum(l_max - k * groups for k in range(per_dev - per_dev // N_CHUNK, per_dev))
        fwd_tab, inv_tab = wave_tables(n_lon, groups, per_dev, N_CHUNK)
        w_rows = w_mix.transpose(0, 1, 3, 2).reshape(l_max * n_chan * 2, n_chan)
        hbm = pl.BlockSpec(memory_space=pltpu.HBM)
        exchange = pltpu.VMEM((N_CHUNK * groups, block, n_chan), BF16)
        dma = pltpu.SemaphoreType.DMA
        out = pl.pallas_call(
            functools.partial(layer_kernel, (groups, n_chan, lat_loc, n_lon, l_max, n_lat, N_CHUNK)),
            out_shape=[pltpu.VMEM((n_chan * lat_loc, LANES), F32)] * (n_lon // LANES),
            in_specs=[hbm] * 6,
            out_specs=[pl.BlockSpec(memory_space=pltpu.VMEM)] * (n_lon // LANES),
            scratch_shapes=[
                pltpu.VMEM((n_lon // LANES, n_chan, lat_loc, LANES), F32),
                pltpu.VMEM((lat_loc // 2, 2 * n_chan, n_lon), BF16),
                pltpu.VMEM((lat_loc, n_chan, n_lon), F32),
                pltpu.VMEM((l_max * n_chan, 2 * n_chan), BF16),
                pltpu.VMEM((4, 8 * n_chan * 2, n_chan), F32),
                pltpu.VMEM((per_dev, l_max, n_lat), F32),
                pltpu.VMEM((per_dev - per_dev // N_CHUNK, l_max, n_lat), F32),
                exchange, exchange, exchange, exchange,
                pltpu.VMEM((n_lat * rows, n_chan), F32),
                pltpu.VMEM((l_max * rows, n_chan), F32),
                pltpu.VMEM((groups, b_rows, 2 * n_chan), BF16),
                pltpu.VMEM((l_max // N_CHUNK, l_max // N_CHUNK, LANES), F32),
                pltpu.VMEM(fwd_tab.shape, BF16),
                pltpu.VMEM(inv_tab.shape, BF16),
                dma((3,)), dma((2, n_lon // LANES)), dma((per_dev,)), dma((per_dev,)), dma((4,)), dma((2 * N_CHUNK,)),
                dma((N_CHUNK, groups)), dma((N_CHUNK, groups)), dma((N_CHUNK + 1, groups)), dma((N_CHUNK + 1, groups)),
                dma((groups // 2,)), dma((groups // 2,)), dma((groups // 2 + 1,)), dma((groups // 2 + 1,)),
            ],
            compiler_params=pltpu.CompilerParams(collective_id=0, has_side_effects=True, vmem_limit_bytes=56 * 2**20),
            name="spectral_layer",
        )(field_loc, p_fwd, p_inv, w_rows, fwd_tab, inv_tab)
        return jnp.concatenate([part.reshape(n_chan, lat_loc, LANES) for part in out], axis=2)

    return jax.shard_map(local_layer, mesh=mesh, in_specs=(P("member", "lat", None), P(), P(), P()), out_specs=P("member", "lat", None), check_vma=False)
```

```python
import functools
import math

import jax
import jax.numpy as jnp
import numpy as np
from jax import lax
from jax.experimental import pallas as pl
from jax.experimental.pallas import tpu as pltpu
from jax.sharding import PartitionSpec as P

MESH = pl.DeviceIdType.MESH
F32 = jnp.float32
BF16 = jnp.bfloat16
LANES = 128
N_CHUNK = 4
PAD = 8


def wave_tables(n_lon, groups, per_dev, n_chunk):
    piece = per_dev // n_chunk
    chunk, dev, part, k = np.meshgrid(np.arange(n_chunk), np.arange(groups), np.arange(2), np.arange(piece), indexing="ij")
    wave = ((chunk * piece + k) * groups + dev).reshape(-1, 1)
    part = part.reshape(-1, 1)
    angle = ((wave * np.arange(n_lon)[None, :]) % n_lon) * (2.0 * math.pi / n_lon)
    fwd = np.where(part == 0, np.cos(angle), -np.sin(angle)).astype(np.float32)
    inv = fwd * np.where(wave == 0, 1.0, 2.0).astype(np.float32)
    return jnp.asarray(fwd, BF16), jnp.asarray(inv, BF16)


def dot(a, b, dims):
    return lax.dot_general(a, b, (dims, ((), ())), preferred_element_type=F32)


def layer_kernel(dims, f_hbm, pw_hbm, pi_hbm, w_hbm, tf_hbm, ti_hbm, *refs):
    n_out = dims[3] // LANES
    o_v, refs = refs[:n_out], refs[n_out:]
    (f_v, f_d, w_v, stage, pw_v, pi_v, f_send, f_recv, g_send, g_recv, wide, coef, b_all, pi_loc, tf_v, ti_v,
                 in_sem, f_sem, pw_sem, pi_sem, w_sem, own_sem, fs_sem, fr_sem, gs_sem, gr_sem, hop_s, hop_r, sib_s, sib_r) = refs
    groups, n_chan, lat_loc, n_lon, l_max, n_lat, n_chunk = dims
    per_dev = l_max // groups
    piece = per_dev // n_chunk
    rows = 2 * piece
    block = lat_loc * rows
    l_step = l_max // n_chunk
    top = n_chunk - 1
    heights = [l_max - (top * piece + i) * groups for i in range(piece)]
    starts = [sum(heights[:i]) for i in range(piece)]
    b_rows = sum(heights)
    member, me = lax.axis_index("member"), lax.axis_index("lat")
    n_z = groups // 2
    z, core = me // 2, lax.rem(me, 2)

    def peer(i):
        step = i // 2
        dist = n_z // 2 - (step + 1) // 2
        dz = jnp.where(lax.rem(step, 2) == 1, dist, -dist)
        far = lax.rem(z + dz + n_z, n_z) * 2 + lax.rem(i, 2)
        return jnp.where(i == groups - 2, z * 2 + 1 - core, far)

    barrier = pltpu.get_barrier_semaphore()

    def greet(i, _):
        pl.semaphore_signal(barrier, inc=1, device_id=(member, peer(i)), device_id_type=MESH)
        return 0

    lax.fori_loop(0, groups - 1, greet, 0)

    n_col = n_lon // LANES

    half = lat_loc // 2

    def f_in(h, x):
        part = pl.ds(h * half, half)
        return pltpu.make_async_copy(f_hbm.at[:, part, pl.ds(x * LANES, LANES)], f_v.at[x, :, part, :], f_sem.at[h, x])

    tf_in = pltpu.make_async_copy(tf_hbm, tf_v, in_sem.at[0])
    ti_in = pltpu.make_async_copy(ti_hbm, ti_v, in_sem.at[1])
    tf_in.start()
    for h in range(2):
        for x in range(n_col):
            f_in(h, x).start()

    def table_copy(src, dst, sem, k):
        low = k * groups
        return pltpu.make_async_copy(src.at[k * groups + me, pl.ds(low, l_max - low), :], dst.at[k, pl.ds(low, l_max - low), :], sem.at[k])

    n_slot = stage.shape[0]
    w_blk = stage.shape[1] // (2 * n_chan)
    n_blk = l_max // w_blk
    blk_rows = stage.shape[1]

    def w_copy(b, slot):
        return pltpu.make_async_copy(w_hbm.at[pl.ds((n_blk - 1 - b) * blk_rows, blk_rows), :], stage.at[slot], w_sem.at[slot])

    lane = me * lat_loc // LANES * LANES
    pi_loc_in = pltpu.make_async_copy(
        pi_hbm.at[pl.ds(top * piece * groups, piece * groups), pl.ds(top * l_step, l_step), pl.ds(pl.multiple_of(lane, LANES), LANES)],
        pi_loc, in_sem.at[2])

    def start_loads():
        for s in range(n_slot):
            w_copy(s, s).start()
        for k in reversed(range(per_dev)):
            table_copy(pw_hbm, pw_v, pw_sem, k).start()
            if k < top * piece:
                table_copy(pi_hbm, pi_v, pi_sem, k).start()
            low, first = k * groups, (k // piece) * l_step
            if low > first:
                pw_v[k, first:low, :] = jnp.zeros((low - first, n_lat), F32)
                if k < top * piece:
                    pi_v[k, first:low, :] = jnp.zeros((low - first, n_lat), F32)
        pi_loc_in.start()
        ti_in.start()

    tf_in.wait()
    tall = lat_loc + PAD
    f_rows = f_v.reshape(n_col, n_chan * tall, LANES)

    def dft_out(j, u, f_pair):
        r = dot(tf_v[j * groups * rows:(j + 1) * groups * rows, :], f_pair, ((1,), (1,)))
        both = [r[:, e * n_chan:(e + 1) * n_chan].reshape(groups, rows, n_chan) for e in range(2)]
        at = pl.ds(pl.multiple_of(u * 2 * rows, 2 * rows), 2 * rows)
        f_send[j * groups:(j + 1) * groups, at, :] = jnp.concatenate(both, axis=1).astype(BF16)

    def dft_first(u, _):
        pair = []
        for e in range(2):
            here = pl.ds(2 * u + e, n_chan, stride=tall)
            f_t = jnp.concatenate([f_rows[x, here, :] for x in range(n_col)], axis=1)
            f_d[2 * u + e] = f_t
            pair.append(f_t.astype(BF16))
        dft_out(top, u, jnp.concatenate(pair, axis=0))
        return 0

    def dft_next(j, u, _):
        f_pair = jnp.concatenate([f_d[2 * u + e].astype(BF16) for e in range(2)], axis=0)
        dft_out(j, u, f_pair)
        return 0

    def fwd_copy(p, to, slot):
        j, part = (p, pl.ds(0, block)) if p < top else (top, pl.ds(0, block // 2))
        if p == n_chunk:
            part = pl.ds(block // 2, block // 2)
        return pltpu.make_async_remote_copy(
            src_ref=f_send.at[j * groups + to, part], dst_ref=f_recv.at[j * groups + slot, part], send_sem=fs_sem.at[p, to],
            recv_sem=fr_sem.at[p, slot], device_id=(member, to), device_id_type=MESH)

    def back_copy(p, to, slot):
        j, part = (p, pl.ds(0, block)) if p else (0, pl.ds(0, block // 2))
        if p == n_chunk:
            j, part = 0, pl.ds(block // 2, block // 2)
        return pltpu.make_async_remote_copy(
            src_ref=g_send.at[j * groups + to, part], dst_ref=g_recv.at[j * groups + slot, part], send_sem=gs_sem.at[p, to],
            recv_sem=gr_sem.at[p, slot], device_id=(member, to), device_id_type=MESH)

    def own_copy(src, dst, j, own):
        return pltpu.make_async_copy(src.at[j * groups + me], dst.at[j * groups + me], own_sem.at[own])

    def send_all(copy, j):
        def go(i, _):
            copy(j, peer(i), me).start()
            return 0

        lax.fori_loop(0, groups - 1, go, 0)

    def recv_all(copy, j):
        def got(i, _):
            s = lax.rem(me + i, groups)
            copy(j, s, s).wait_recv()
            return 0

        lax.fori_loop(1, groups, got, 0)

    def sent_all(copy, j):
        def done(i, _):
            s = lax.rem(me + i, groups)
            copy(j, s, s).wait_send()
            return 0

        lax.fori_loop(1, groups, done, 0)

    n_hop = n_z // 2

    def b_part(h, sgn):
        if h < n_hop:
            return pl.ds(0, b_rows)
        return pl.ds(0 if sgn > 0 else b_rows // 2, b_rows // 2)

    def chip(dz):
        return lax.rem(z + dz + n_z, n_z)

    def b_remote(s, part, to, sems, n):
        return pltpu.make_async_remote_copy(
            src_ref=b_all.at[s, part], dst_ref=b_all.at[s, part], send_sem=sems[0].at[n], recv_sem=sems[1].at[n],
            device_id=(member, to), device_id_type=MESH)

    def hop(h, sgn, arriving):
        s = chip(-sgn * (h if arriving else h - 1)) * 2 + core
        n = (h - 1) * 2 + (sgn < 0)
        return b_remote(s, b_part(h, sgn), chip(sgn) * 2 + core, (hop_s, hop_r), n)

    def sib(h, sgn, arriving):
        s = chip(-sgn * h) * 2 + (1 - core if arriving else core)
        n = 0 if h == 0 else (h - 1) * 2 + (sgn < 0) + 1
        return b_remote(s, b_part(h, sgn), z * 2 + 1 - core, (sib_s, sib_r), n)

    hops = [(h, sgn) for h in range(1, n_hop + 1) for sgn in (1, -1)]

    def relay(h):
        for sgn in (1, -1):
            if h > 0:
                hop(h, sgn, True).wait_recv()
            if h < n_hop:
                hop(h + 1, sgn, False).start()
            if h > 0 or sgn > 0:
                sib(h, sgn, False).start()

    def b_done():
        for h, sgn in hops:
            hop(h, sgn, False).wait_send()
        for h, sgn in [(0, 1)] + hops:
            sib(h, sgn, False).wait_send()

    order = list(reversed(range(n_chunk)))

    def send_fwd(j):
        own_copy(f_send, f_recv, j, j).start()
        send_all(fwd_copy, j)

    def send_back(j):
        own_copy(g_send, g_recv, j, n_chunk + j).start()
        send_all(back_copy, j)
        if j == 0:
            send_all(back_copy, n_chunk)

    for h in range(2):
        for x in range(n_col):
            f_in(h, x).wait()
        if h == 1:
            start_loads()
        lax.fori_loop(h * half // 2, (h + 1) * half // 2, dft_first, 0, unroll=2)
        if h == 0:
            pl.semaphore_wait(barrier, groups - 1)
            send_all(fwd_copy, top)
    own_copy(f_send, f_recv, top, top).start()
    send_all(fwd_copy, n_chunk)
    for j in order[1:]:
        lax.fori_loop(0, lat_loc // 2, functools.partial(dft_next, j), 0, unroll=2)
        if j == top - 1:
            send_fwd(j)

    sign = jnp.where(lax.broadcasted_iota(jnp.int32, (rows, n_chan), 0) < piece, -1.0, 1.0).astype(F32)

    def load_w(b, _):
        slot = lax.rem(b, n_slot)
        w_copy(b, slot).wait()
        half = blk_rows // 2
        re = stage[slot, pl.ds(0, half, stride=2), :]
        im = stage[slot, pl.ds(1, half, stride=2), :]
        at = pl.ds(pl.multiple_of((n_blk - 1 - b) * half, half), half)
        w_v[at, :n_chan] = re.astype(BF16)
        w_v[at, n_chan:] = im.astype(BF16)

        @pl.when(b + n_slot < n_blk)
        def _():
            w_copy(b + n_slot, slot).start()

        return 0

    blk_chunk = n_blk // n_chunk
    n_row = n_lat * rows
    for at, j in enumerate(order):
        lax.fori_loop(at * blk_chunk, (at + 1) * blk_chunk, load_w, 0)
        own_copy(f_send, f_recv, j, j).wait()
        recv_all(fwd_copy, j)
        if j == top:
            recv_all(fwd_copy, n_chunk)
        low = j * l_step
        n_l = l_max - low

        def widen(s, _):
            wide[pl.ds(pl.multiple_of(s * block, block), block), :] = f_recv[j * groups + s].astype(F32)
            return 0

        lax.fori_loop(0, groups, widen, 0)
        for i in range(piece):
            k = j * piece + i
            table_copy(pw_hbm, pw_v, pw_sem, k).wait()
            re = wide[pl.ds(i, n_lat, stride=rows), :]
            im = wide[pl.ds(piece + i, n_lat, stride=rows), :]
            spec = jnp.concatenate([re, im], axis=1).astype(BF16)
            a = dot(pw_v[k, low:, :].astype(BF16), spec, ((1,), (0,)))
            coef[pl.ds(low * rows + i, n_l, stride=rows), :] = a[:, :n_chan]
            coef[pl.ds(low * rows + piece + i, n_l, stride=rows), :] = a[:, n_chan:]

        def mix(v, _):
            for e in range(8):
                deg = v * 8 + e
                here = pl.ds(pl.multiple_of(deg * rows, rows), rows)
                w_l = w_v[pl.ds(pl.multiple_of(deg * n_chan, n_chan), n_chan), :]
                r = dot(coef[here, :].astype(BF16), w_l, ((1,), (0,)))
                coef[here, :] = r[:, :n_chan] + sign * pltpu.roll(r[:, n_chan:], piece, 0)
            return 0

        lax.fori_loop(low // 8, l_max // 8, mix, 0)
        if j == top:
            for i in range(piece):
                n_i = heights[i]
                base = (l_max - n_i) * rows
                re = coef[pl.ds(base + i, n_i, stride=rows), :]
                im = coef[pl.ds(base + piece + i, n_i, stride=rows), :]
                b_all[me, starts[i]:starts[i] + n_i, :] = jnp.concatenate([re, im], axis=1).astype(BF16)
            relay(0)
            send_fwd(top - 2)
            continue
        for i in range(piece):
            k = j * piece + i
            table_copy(pi_hbm, pi_v, pi_sem, k).wait()
            re = coef[pl.ds(low * rows + i, n_l, stride=rows), :]
            im = coef[pl.ds(low * rows + piece + i, n_l, stride=rows), :]
            b = jnp.concatenate([re, im], axis=1).astype(BF16)
            g = dot(pi_v[k, low:, :].astype(BF16), b, ((0,), (0,)))
            wide[pl.ds(i, n_lat, stride=rows), :] = g[:, :n_chan]
            wide[pl.ds(piece + i, n_lat, stride=rows), :] = g[:, n_chan:]

        def narrow(s, _):
            g_send[j * groups + s] = wide[pl.ds(pl.multiple_of(s * block, block), block), :].astype(BF16)
            return 0

        lax.fori_loop(0, groups, narrow, 0)
        relay(top - j)
        if j == top - 1:
            send_fwd(0)
        if j == top - 2:
            send_back(top - 1)
        if j == 0:
            send_back(1)
            send_back(0)

    def own_rows(d, _):
        for i in range(piece):
            n_i = heights[i]
            p_i = pltpu.roll(pi_loc[i * groups + d, l_step - n_i:, :], lax.rem(lane + LANES - me * lat_loc, LANES), 1)
            g = dot(p_i.T[:lat_loc].astype(BF16), b_all[d, starts[i]:starts[i] + n_i, :], ((1,), (0,)))
            wide[pl.ds(d * block + i, lat_loc, stride=rows), :] = g[:, :n_chan]
            wide[pl.ds(d * block + piece + i, lat_loc, stride=rows), :] = g[:, n_chan:]
        g_recv[top * groups + d] = wide[pl.ds(pl.multiple_of(d * block, block), block), :].astype(BF16)
        return 0

    ti_in.wait()
    back_order = [top - 1, top] + order[2:]
    for at, j in enumerate(back_order):
        if j == top:
            relay(n_hop)
            for h, sgn in [(0, 1)] + hops:
                sib(h, sgn, True).wait_recv()
            pi_loc_in.wait()
            lax.fori_loop(0, groups, own_rows, 0)
        else:
            own_copy(g_send, g_recv, j, n_chunk + j).wait()
            recv_all(back_copy, j)
        last = at == n_chunk - 1

        def inverse(u, _):
            pair = g_recv[j * groups:(j + 1) * groups, pl.ds(pl.multiple_of(u * 2 * rows, 2 * rows), 2 * rows), :].astype(F32)
            for half in range(2):
                t = 2 * u + half
                g_t = pair[:, half * rows:(half + 1) * rows, :].reshape(groups * rows, n_chan)
                h = dot(g_t.T.astype(BF16), ti_v[j * groups * rows:(j + 1) * groups * rows, :], ((1,), (0,)))
                kept = pl.ds(pl.multiple_of(t * n_chan, n_chan), n_chan)
                for x in range(n_col):
                    lanes = slice(x * LANES, (x + 1) * LANES)
                    h_x = h[:, lanes]
                    if at > 0:
                        h_x = h_x + f_rows[x, kept, :]
                    if last:
                        o_v[x][pl.ds(t, n_chan, stride=tall), :] = f_d[t, :, lanes] + jax.nn.gelu(h_x)
                    else:
                        f_rows[x, kept, :] = h_x
            return 0

        if last:
            lax.fori_loop(0, lat_loc // 4, inverse, 0)
            recv_all(back_copy, n_chunk)
            lax.fori_loop(lat_loc // 4, lat_loc // 2, inverse, 0)
        else:
            lax.fori_loop(0, lat_loc // 2, inverse, 0)
    for j in order:
        sent_all(fwd_copy, j)
        if j < top:
            sent_all(back_copy, j)
    b_done()
    sent_all(fwd_copy, n_chunk)
    sent_all(back_copy, n_chunk)


def solution(mesh):
    groups = mesh.shape["lat"]

    def local_layer(field_loc, p_fwd, p_inv, w_mix):
        n_chan, lat_loc, n_lon = field_loc.shape
        l_max, _, n_lat = p_fwd.shape
        per_dev = l_max // groups
        rows = 2 * per_dev // N_CHUNK
        block = lat_loc * rows
        b_rows = sum(l_max - k * groups for k in range(per_dev - per_dev // N_CHUNK, per_dev))
        fwd_tab, inv_tab = wave_tables(n_lon, groups, per_dev, N_CHUNK)
        w_rows = w_mix.transpose(0, 1, 3, 2).reshape(l_max * n_chan * 2, n_chan)
        hbm = pl.BlockSpec(memory_space=pltpu.HBM)
        exchange = pltpu.VMEM((N_CHUNK * groups, block, n_chan), BF16)
        dma = pltpu.SemaphoreType.DMA
        out = pl.pallas_call(
            functools.partial(layer_kernel, (groups, n_chan, lat_loc, n_lon, l_max, n_lat, N_CHUNK)),
            out_shape=[pltpu.VMEM((n_chan * (lat_loc + PAD), LANES), F32)] * (n_lon // LANES),
            in_specs=[hbm] * 6,
            out_specs=[pl.BlockSpec(memory_space=pltpu.VMEM)] * (n_lon // LANES),
            scratch_shapes=[
                pltpu.VMEM((n_lon // LANES, n_chan, lat_loc + PAD, LANES), F32),
                pltpu.VMEM((lat_loc, n_chan, n_lon), F32),
                pltpu.VMEM((l_max * n_chan, 2 * n_chan), BF16),
                pltpu.VMEM((4, 8 * n_chan * 2, n_chan), F32),
                pltpu.VMEM((per_dev, l_max, n_lat), F32),
                pltpu.VMEM((per_dev - per_dev // N_CHUNK, l_max, n_lat), F32),
                exchange, exchange, exchange, exchange,
                pltpu.VMEM((n_lat * rows, n_chan), F32),
                pltpu.VMEM((l_max * rows, n_chan), F32),
                pltpu.VMEM((groups, b_rows, 2 * n_chan), BF16),
                pltpu.VMEM((l_max // N_CHUNK, l_max // N_CHUNK, LANES), F32),
                pltpu.VMEM(fwd_tab.shape, BF16),
                pltpu.VMEM(inv_tab.shape, BF16),
                dma((3,)), dma((2, n_lon // LANES)), dma((per_dev,)), dma((per_dev,)), dma((4,)), dma((2 * N_CHUNK,)),
                dma((N_CHUNK + 1, groups)), dma((N_CHUNK + 1, groups)), dma((N_CHUNK + 1, groups)), dma((N_CHUNK + 1, groups)),
                dma((groups // 2,)), dma((groups // 2,)), dma((groups // 2 + 1,)), dma((groups // 2 + 1,)),
            ],
            compiler_params=pltpu.CompilerParams(collective_id=0, has_side_effects=True, vmem_limit_bytes=56 * 2**20),
            name="spectral_layer",
        )(field_loc, p_fwd, p_inv, w_rows, fwd_tab, inv_tab)
        return jnp.concatenate([part.reshape(n_chan, lat_loc + PAD, LANES)[:, :lat_loc] for part in out], axis=2)

    return jax.shard_map(local_layer, mesh=mesh, in_specs=(P("member", "lat", None), P(), P(), P()), out_specs=P("member", "lat", None), check_vma=False)
```

```python
import functools
import math

import jax
import jax.numpy as jnp
import numpy as np
from jax import lax
from jax.experimental import pallas as pl
from jax.experimental.pallas import tpu as pltpu
from jax.sharding import PartitionSpec as P

MESH = pl.DeviceIdType.MESH
F32 = jnp.float32
BF16 = jnp.bfloat16
LANES = 128
N_CHUNK = 4
PAD = 8


def wave_tables(n_lon, groups, per_dev, n_chunk):
    piece = per_dev // n_chunk
    chunk, dev, part, k = np.meshgrid(np.arange(n_chunk), np.arange(groups), np.arange(2), np.arange(piece), indexing="ij")
    wave = ((chunk * piece + k) * groups + dev).reshape(-1, 1)
    part = part.reshape(-1, 1)
    angle = ((wave * np.arange(n_lon)[None, :]) % n_lon) * (2.0 * math.pi / n_lon)
    fwd = np.where(part == 0, np.cos(angle), -np.sin(angle)).astype(np.float32)
    inv = fwd * np.where(wave == 0, 1.0, 2.0).astype(np.float32)
    return jnp.asarray(fwd, BF16), jnp.asarray(inv, BF16)


def dot(a, b, dims):
    return lax.dot_general(a, b, (dims, ((), ())), preferred_element_type=F32)


def layer_kernel(dims, f_hbm, pw_hbm, pi_hbm, w_hbm, tf_hbm, ti_hbm, *refs):
    n_out = dims[3] // LANES
    o_v, refs = refs[:n_out], refs[n_out:]
    (f_v, f_d, w_v, stage, pw_v, pi_v, f_send, f_recv, g_send, g_recv, wide, coef, b_all, pi_loc, tf_v, ti_v,
                 in_sem, f_sem, pw_sem, pi_sem, w_sem, own_sem, fs_sem, fr_sem, gs_sem, gr_sem, hop_s, hop_r, sib_s, sib_r) = refs
    groups, n_chan, lat_loc, n_lon, l_max, n_lat, n_chunk = dims
    per_dev = l_max // groups
    piece = per_dev // n_chunk
    rows = 2 * piece
    block = lat_loc * rows
    n_first = block * 3 // 4
    l_step = l_max // n_chunk
    top = n_chunk - 1
    heights = [l_max - (top * piece + i) * groups for i in range(piece)]
    starts = [sum(heights[:i]) for i in range(piece)]
    b_rows = sum(heights)
    member, me = lax.axis_index("member"), lax.axis_index("lat")
    n_z = groups // 2
    z, core = me // 2, lax.rem(me, 2)

    def peer(i):
        step = i // 2
        dist = n_z // 2 - (step + 1) // 2
        dz = jnp.where(lax.rem(step, 2) == 1, dist, -dist)
        far = lax.rem(z + dz + n_z, n_z) * 2 + lax.rem(i, 2)
        return jnp.where(i == groups - 2, z * 2 + 1 - core, far)

    barrier = pltpu.get_barrier_semaphore()

    def greet(i, _):
        pl.semaphore_signal(barrier, inc=1, device_id=(member, peer(i)), device_id_type=MESH)
        return 0

    lax.fori_loop(0, groups - 1, greet, 0)

    n_col = n_lon // LANES

    half = lat_loc // 2

    def f_in(h, x):
        part = pl.ds(h * half, half)
        return pltpu.make_async_copy(f_hbm.at[:, part, pl.ds(x * LANES, LANES)], f_v.at[x, :, part, :], f_sem.at[h, x])

    tf_in = pltpu.make_async_copy(tf_hbm, tf_v, in_sem.at[0])
    ti_in = pltpu.make_async_copy(ti_hbm, ti_v, in_sem.at[1])
    tf_in.start()
    for h in range(2):
        for x in range(n_col):
            f_in(h, x).start()

    def table_copy(src, dst, sem, k):
        low = k * groups
        return pltpu.make_async_copy(src.at[k * groups + me, pl.ds(low, l_max - low), :], dst.at[k, pl.ds(low, l_max - low), :], sem.at[k])

    n_slot = stage.shape[0]
    w_blk = stage.shape[1] // (2 * n_chan)
    n_blk = l_max // w_blk
    blk_rows = stage.shape[1]

    def w_copy(b, slot):
        return pltpu.make_async_copy(w_hbm.at[pl.ds((n_blk - 1 - b) * blk_rows, blk_rows), :], stage.at[slot], w_sem.at[slot])

    lane = me * lat_loc // LANES * LANES
    pi_loc_in = pltpu.make_async_copy(
        pi_hbm.at[pl.ds(top * piece * groups, piece * groups), pl.ds(top * l_step, l_step), pl.ds(pl.multiple_of(lane, LANES), LANES)],
        pi_loc, in_sem.at[2])

    def start_loads():
        for s in range(n_slot):
            w_copy(s, s).start()
        for k in reversed(range(per_dev)):
            table_copy(pw_hbm, pw_v, pw_sem, k).start()
            if k < top * piece:
                table_copy(pi_hbm, pi_v, pi_sem, k).start()
            low, first = k * groups, (k // piece) * l_step
            if low > first:
                pw_v[k, first:low, :] = jnp.zeros((low - first, n_lat), F32)
                if k < top * piece:
                    pi_v[k, first:low, :] = jnp.zeros((low - first, n_lat), F32)
        pi_loc_in.start()
        ti_in.start()

    tf_in.wait()
    tall = lat_loc + PAD
    f_rows = f_v.reshape(n_col, n_chan * tall, LANES)

    def dft_out(j, u, f_pair):
        r = dot(tf_v[j * groups * rows:(j + 1) * groups * rows, :], f_pair, ((1,), (1,)))
        both = [r[:, e * n_chan:(e + 1) * n_chan].reshape(groups, rows, n_chan) for e in range(2)]
        at = pl.ds(pl.multiple_of(u * 2 * rows, 2 * rows), 2 * rows)
        f_send[j * groups:(j + 1) * groups, at, :] = jnp.concatenate(both, axis=1).astype(BF16)

    def dft_first(u, _):
        pair = []
        for e in range(2):
            here = pl.ds(2 * u + e, n_chan, stride=tall)
            f_t = jnp.concatenate([f_rows[x, here, :] for x in range(n_col)], axis=1)
            f_d[2 * u + e] = f_t
            pair.append(f_t.astype(BF16))
        dft_out(top, u, jnp.concatenate(pair, axis=0))
        return 0

    def dft_next(j, u, _):
        f_pair = jnp.concatenate([f_d[2 * u + e].astype(BF16) for e in range(2)], axis=0)
        dft_out(j, u, f_pair)
        return 0

    def fwd_copy(p, to, slot):
        j, part = (p, pl.ds(0, block)) if p < top else (top, pl.ds(0, block // 2))
        if p == n_chunk:
            part = pl.ds(block // 2, block // 2)
        return pltpu.make_async_remote_copy(
            src_ref=f_send.at[j * groups + to, part], dst_ref=f_recv.at[j * groups + slot, part], send_sem=fs_sem.at[p, to],
            recv_sem=fr_sem.at[p, slot], device_id=(member, to), device_id_type=MESH)

    def back_copy(p, to, slot):
        j, part = (p, pl.ds(0, block)) if p else (0, pl.ds(0, n_first))
        if p == n_chunk:
            j, part = 0, pl.ds(n_first, block - n_first)
        return pltpu.make_async_remote_copy(
            src_ref=g_send.at[j * groups + to, part], dst_ref=g_recv.at[j * groups + slot, part], send_sem=gs_sem.at[p, to],
            recv_sem=gr_sem.at[p, slot], device_id=(member, to), device_id_type=MESH)

    def own_copy(src, dst, j, own):
        return pltpu.make_async_copy(src.at[j * groups + me], dst.at[j * groups + me], own_sem.at[own])

    def send_all(copy, j):
        def go(i, _):
            copy(j, peer(i), me).start()
            return 0

        lax.fori_loop(0, groups - 1, go, 0)

    def recv_all(copy, j):
        def got(i, _):
            s = lax.rem(me + i, groups)
            copy(j, s, s).wait_recv()
            return 0

        lax.fori_loop(1, groups, got, 0)

    def sent_all(copy, j):
        def done(i, _):
            s = lax.rem(me + i, groups)
            copy(j, s, s).wait_send()
            return 0

        lax.fori_loop(1, groups, done, 0)

    n_hop = n_z // 2

    def b_part(h, sgn):
        if h < n_hop:
            return pl.ds(0, b_rows)
        return pl.ds(0 if sgn > 0 else b_rows // 2, b_rows // 2)

    def chip(dz):
        return lax.rem(z + dz + n_z, n_z)

    def b_remote(s, part, to, sems, n):
        return pltpu.make_async_remote_copy(
            src_ref=b_all.at[s, part], dst_ref=b_all.at[s, part], send_sem=sems[0].at[n], recv_sem=sems[1].at[n],
            device_id=(member, to), device_id_type=MESH)

    def hop(h, sgn, arriving):
        s = chip(-sgn * (h if arriving else h - 1)) * 2 + core
        n = (h - 1) * 2 + (sgn < 0)
        return b_remote(s, b_part(h, sgn), chip(sgn) * 2 + core, (hop_s, hop_r), n)

    def sib(h, sgn, arriving):
        s = chip(-sgn * h) * 2 + (1 - core if arriving else core)
        n = 0 if h == 0 else (h - 1) * 2 + (sgn < 0) + 1
        return b_remote(s, b_part(h, sgn), z * 2 + 1 - core, (sib_s, sib_r), n)

    hops = [(h, sgn) for h in range(1, n_hop + 1) for sgn in (1, -1)]

    def relay(h):
        for sgn in (1, -1):
            if h > 0:
                hop(h, sgn, True).wait_recv()
            if h < n_hop:
                hop(h + 1, sgn, False).start()
            if h > 0 or sgn > 0:
                sib(h, sgn, False).start()

    def b_done():
        for h, sgn in hops:
            hop(h, sgn, False).wait_send()
        for h, sgn in [(0, 1)] + hops:
            sib(h, sgn, False).wait_send()

    order = list(reversed(range(n_chunk)))

    def send_fwd(j):
        own_copy(f_send, f_recv, j, j).start()
        send_all(fwd_copy, j)

    def send_back(j):
        own_copy(g_send, g_recv, j, n_chunk + j).start()
        send_all(back_copy, j)
        if j == 0:
            send_all(back_copy, n_chunk)

    for h in range(2):
        for x in range(n_col):
            f_in(h, x).wait()
        if h == 1:
            start_loads()
        lax.fori_loop(h * half // 2, (h + 1) * half // 2, dft_first, 0, unroll=2)
        if h == 0:
            pl.semaphore_wait(barrier, groups - 1)
            send_all(fwd_copy, top)
    own_copy(f_send, f_recv, top, top).start()
    send_all(fwd_copy, n_chunk)
    for j in order[1:]:
        lax.fori_loop(0, lat_loc // 2, functools.partial(dft_next, j), 0, unroll=2)
        if j == top - 1:
            send_fwd(j)

    sign = jnp.where(lax.broadcasted_iota(jnp.int32, (rows, n_chan), 0) < piece, -1.0, 1.0).astype(F32)

    def load_w(b, _):
        slot = lax.rem(b, n_slot)
        w_copy(b, slot).wait()
        half = blk_rows // 2
        re = stage[slot, pl.ds(0, half, stride=2), :]
        im = stage[slot, pl.ds(1, half, stride=2), :]
        at = pl.ds(pl.multiple_of((n_blk - 1 - b) * half, half), half)
        w_v[at, :n_chan] = re.astype(BF16)
        w_v[at, n_chan:] = im.astype(BF16)

        @pl.when(b + n_slot < n_blk)
        def _():
            w_copy(b + n_slot, slot).start()

        return 0

    blk_chunk = n_blk // n_chunk
    n_row = n_lat * rows
    for at, j in enumerate(order):
        lax.fori_loop(at * blk_chunk, (at + 1) * blk_chunk, load_w, 0)
        own_copy(f_send, f_recv, j, j).wait()
        recv_all(fwd_copy, j)
        if j == top:
            recv_all(fwd_copy, n_chunk)
        low = j * l_step
        n_l = l_max - low

        def widen(s, _):
            wide[pl.ds(pl.multiple_of(s * block, block), block), :] = f_recv[j * groups + s].astype(F32)
            return 0

        lax.fori_loop(0, groups, widen, 0)
        for i in range(piece):
            k = j * piece + i
            table_copy(pw_hbm, pw_v, pw_sem, k).wait()
            re = wide[pl.ds(i, n_lat, stride=rows), :]
            im = wide[pl.ds(piece + i, n_lat, stride=rows), :]
            spec = jnp.concatenate([re, im], axis=1).astype(BF16)
            a = dot(pw_v[k, low:, :].astype(BF16), spec, ((1,), (0,)))
            coef[pl.ds(low * rows + i, n_l, stride=rows), :] = a[:, :n_chan]
            coef[pl.ds(low * rows + piece + i, n_l, stride=rows), :] = a[:, n_chan:]

        def mix(v, _):
            for e in range(8):
                deg = v * 8 + e
                here = pl.ds(pl.multiple_of(deg * rows, rows), rows)
                w_l = w_v[pl.ds(pl.multiple_of(deg * n_chan, n_chan), n_chan), :]
                r = dot(coef[here, :].astype(BF16), w_l, ((1,), (0,)))
                coef[here, :] = r[:, :n_chan] + sign * pltpu.roll(r[:, n_chan:], piece, 0)
            return 0

        lax.fori_loop(low // 8, l_max // 8, mix, 0)
        if j == top:
            for i in range(piece):
                n_i = heights[i]
                base = (l_max - n_i) * rows
                re = coef[pl.ds(base + i, n_i, stride=rows), :]
                im = coef[pl.ds(base + piece + i, n_i, stride=rows), :]
                b_all[me, starts[i]:starts[i] + n_i, :] = jnp.concatenate([re, im], axis=1).astype(BF16)
            relay(0)
            send_fwd(top - 2)
            continue
        for i in range(piece):
            k = j * piece + i
            table_copy(pi_hbm, pi_v, pi_sem, k).wait()
            re = coef[pl.ds(low * rows + i, n_l, stride=rows), :]
            im = coef[pl.ds(low * rows + piece + i, n_l, stride=rows), :]
            b = jnp.concatenate([re, im], axis=1).astype(BF16)
            g = dot(pi_v[k, low:, :].astype(BF16), b, ((0,), (0,)))
            wide[pl.ds(i, n_lat, stride=rows), :] = g[:, :n_chan]
            wide[pl.ds(piece + i, n_lat, stride=rows), :] = g[:, n_chan:]

        def narrow(s, _):
            g_send[j * groups + s] = wide[pl.ds(pl.multiple_of(s * block, block), block), :].astype(BF16)
            return 0

        lax.fori_loop(0, groups, narrow, 0)
        relay(top - j)
        if j == top - 1:
            send_fwd(0)
        if j == top - 2:
            send_back(top - 1)
        if j == 0:
            send_back(1)
            send_back(0)

    def own_rows(d, _):
        for i in range(piece):
            n_i = heights[i]
            p_i = pltpu.roll(pi_loc[i * groups + d, l_step - n_i:, :], lax.rem(lane + LANES - me * lat_loc, LANES), 1)
            g = dot(p_i.T[:lat_loc].astype(BF16), b_all[d, starts[i]:starts[i] + n_i, :], ((1,), (0,)))
            wide[pl.ds(d * block + i, lat_loc, stride=rows), :] = g[:, :n_chan]
            wide[pl.ds(d * block + piece + i, lat_loc, stride=rows), :] = g[:, n_chan:]
        g_recv[top * groups + d] = wide[pl.ds(pl.multiple_of(d * block, block), block), :].astype(BF16)
        return 0

    ti_in.wait()
    back_order = [top - 1, top] + order[2:]
    for at, j in enumerate(back_order):
        if j == top:
            relay(n_hop)
            for h, sgn in [(0, 1)] + hops:
                sib(h, sgn, True).wait_recv()
            pi_loc_in.wait()
            lax.fori_loop(0, groups, own_rows, 0)
        else:
            own_copy(g_send, g_recv, j, n_chunk + j).wait()
            recv_all(back_copy, j)
        last = at == n_chunk - 1

        def inverse(u, _):
            pair = g_recv[j * groups:(j + 1) * groups, pl.ds(pl.multiple_of(u * 2 * rows, 2 * rows), 2 * rows), :].astype(F32)
            for half in range(2):
                t = 2 * u + half
                g_t = pair[:, half * rows:(half + 1) * rows, :].reshape(groups * rows, n_chan)
                h = dot(g_t.T.astype(BF16), ti_v[j * groups * rows:(j + 1) * groups * rows, :], ((1,), (0,)))
                kept = pl.ds(pl.multiple_of(t * n_chan, n_chan), n_chan)
                for x in range(n_col):
                    lanes = slice(x * LANES, (x + 1) * LANES)
                    h_x = h[:, lanes]
                    if at > 0:
                        h_x = h_x + f_rows[x, kept, :]
                    if last:
                        o_v[x][pl.ds(t, n_chan, stride=tall), :] = f_d[t, :, lanes] + jax.nn.gelu(h_x)
                    else:
                        f_rows[x, kept, :] = h_x
            return 0

        if last:
            first = n_first // rows // 2
            lax.fori_loop(0, first, inverse, 0, unroll=2)
            recv_all(back_copy, n_chunk)
            lax.fori_loop(first, lat_loc // 2, inverse, 0, unroll=2)
        else:
            lax.fori_loop(0, lat_loc // 2, inverse, 0)
    for j in order:
        sent_all(fwd_copy, j)
        if j < top:
            sent_all(back_copy, j)
    b_done()
    sent_all(fwd_copy, n_chunk)
    sent_all(back_copy, n_chunk)


def out_kernel(n_chan, lat_loc, *refs):
    parts, o_hbm, sem = refs[:-2], refs[-2], refs[-1]
    copies = []
    for x, part in enumerate(parts):
        rows = part.reshape(n_chan, part.shape[0] // n_chan, LANES).at[:, pl.ds(0, lat_loc), :]
        copies.append(pltpu.make_async_copy(rows, o_hbm.at[:, :, pl.ds(x * LANES, LANES)], sem.at[x]))
    for copy in copies:
        copy.start()
    for copy in copies:
        copy.wait()


def solution(mesh):
    groups = mesh.shape["lat"]

    def local_layer(field_loc, p_fwd, p_inv, w_mix):
        n_chan, lat_loc, n_lon = field_loc.shape
        l_max, _, n_lat = p_fwd.shape
        per_dev = l_max // groups
        rows = 2 * per_dev // N_CHUNK
        block = lat_loc * rows
        b_rows = sum(l_max - k * groups for k in range(per_dev - per_dev // N_CHUNK, per_dev))
        fwd_tab, inv_tab = wave_tables(n_lon, groups, per_dev, N_CHUNK)
        w_rows = w_mix.transpose(0, 1, 3, 2).reshape(l_max * n_chan * 2, n_chan)
        hbm = pl.BlockSpec(memory_space=pltpu.HBM)
        exchange = pltpu.VMEM((N_CHUNK * groups, block, n_chan), BF16)
        dma = pltpu.SemaphoreType.DMA
        out = pl.pallas_call(
            functools.partial(layer_kernel, (groups, n_chan, lat_loc, n_lon, l_max, n_lat, N_CHUNK)),
            out_shape=[pltpu.VMEM((n_chan * (lat_loc + PAD), LANES), F32)] * (n_lon // LANES),
            in_specs=[hbm] * 6,
            out_specs=[pl.BlockSpec(memory_space=pltpu.VMEM)] * (n_lon // LANES),
            scratch_shapes=[
                pltpu.VMEM((n_lon // LANES, n_chan, lat_loc + PAD, LANES), F32),
                pltpu.VMEM((lat_loc, n_chan, n_lon), F32),
                pltpu.VMEM((l_max * n_chan, 2 * n_chan), BF16),
                pltpu.VMEM((4, 8 * n_chan * 2, n_chan), F32),
                pltpu.VMEM((per_dev, l_max, n_lat), F32),
                pltpu.VMEM((per_dev - per_dev // N_CHUNK, l_max, n_lat), F32),
                exchange, exchange, exchange, exchange,
                pltpu.VMEM((n_lat * rows, n_chan), F32),
                pltpu.VMEM((l_max * rows, n_chan), F32),
                pltpu.VMEM((groups, b_rows, 2 * n_chan), BF16),
                pltpu.VMEM((l_max // N_CHUNK, l_max // N_CHUNK, LANES), F32),
                pltpu.VMEM(fwd_tab.shape, BF16),
                pltpu.VMEM(inv_tab.shape, BF16),
                dma((3,)), dma((2, n_lon // LANES)), dma((per_dev,)), dma((per_dev,)), dma((4,)), dma((2 * N_CHUNK,)),
                dma((N_CHUNK + 1, groups)), dma((N_CHUNK + 1, groups)), dma((N_CHUNK + 1, groups)), dma((N_CHUNK + 1, groups)),
                dma((groups // 2,)), dma((groups // 2,)), dma((groups // 2 + 1,)), dma((groups // 2 + 1,)),
            ],
            compiler_params=pltpu.CompilerParams(collective_id=0, has_side_effects=True, vmem_limit_bytes=56 * 2**20),
            name="spectral_layer",
        )(field_loc, p_fwd, p_inv, w_rows, fwd_tab, inv_tab)
        vmem = pl.BlockSpec(memory_space=pltpu.VMEM)
        return pl.pallas_call(
            functools.partial(out_kernel, n_chan, lat_loc),
            out_shape=jax.ShapeDtypeStruct(field_loc.shape, F32),
            in_specs=[vmem] * len(out),
            out_specs=hbm,
            scratch_shapes=[dma((len(out),))],
            compiler_params=pltpu.CompilerParams(vmem_limit_bytes=2**20),
            name="result_out",
        )(*out)

    return jax.shard_map(local_layer, mesh=mesh, in_specs=(P("member", "lat", None), P(), P(), P()), out_specs=P("member", "lat", None), check_vma=False)
```

```python
import functools
import math

import jax
import jax.numpy as jnp
import numpy as np
from jax import lax
from jax.experimental import pallas as pl
from jax.experimental.pallas import tpu as pltpu
from jax.sharding import PartitionSpec as P

MESH = pl.DeviceIdType.MESH
F32 = jnp.float32
BF16 = jnp.bfloat16
LANES = 128
N_CHUNK = 4
PAD = 8


def wave_tables(n_lon, groups, per_dev, n_chunk):
    piece = per_dev // n_chunk
    chunk, dev, part, k = np.meshgrid(np.arange(n_chunk), np.arange(groups), np.arange(2), np.arange(piece), indexing="ij")
    wave = ((chunk * piece + k) * groups + dev).reshape(-1, 1)
    part = part.reshape(-1, 1)
    angle = ((wave * np.arange(n_lon)[None, :]) % n_lon) * (2.0 * math.pi / n_lon)
    fwd = np.where(part == 0, np.cos(angle), -np.sin(angle)).astype(np.float32)
    inv = fwd * np.where(wave == 0, 1.0, 2.0).astype(np.float32)
    return jnp.asarray(fwd, BF16), jnp.asarray(inv, BF16)


def dot(a, b, dims):
    return lax.dot_general(a, b, (dims, ((), ())), preferred_element_type=F32)


def layer_kernel(dims, f_hbm, pw_hbm, pi_hbm, w_hbm, tf_hbm, ti_hbm, *refs):
    n_out = dims[3] // LANES
    o_v, refs = refs[:n_out], refs[n_out:]
    (f_v, f_d, w_v, stage, pw_v, pi_v, f_send, f_recv, g_send, g_recv, wide, coef, b_all, pi_loc, tf_v, ti_v,
                 in_sem, f_sem, pw_sem, pi_sem, w_sem, own_sem, fs_sem, fr_sem, gs_sem, gr_sem, hop_s, hop_r, sib_s, sib_r) = refs
    groups, n_chan, lat_loc, n_lon, l_max, n_lat, n_chunk = dims
    per_dev = l_max // groups
    piece = per_dev // n_chunk
    rows = 2 * piece
    block = lat_loc * rows
    n_first = block * 3 // 4
    l_step = l_max // n_chunk
    top = n_chunk - 1
    heights = [l_max - (top * piece + i) * groups for i in range(piece)]
    starts = [sum(heights[:i]) for i in range(piece)]
    b_rows = sum(heights)
    member, me = lax.axis_index("member"), lax.axis_index("lat")
    n_z = groups // 2
    z, core = me // 2, lax.rem(me, 2)

    def peer(i):
        step = i // 2
        dist = n_z // 2 - (step + 1) // 2
        dz = jnp.where(lax.rem(step, 2) == 1, dist, -dist)
        far = lax.rem(z + dz + n_z, n_z) * 2 + lax.rem(i, 2)
        return jnp.where(i == groups - 2, z * 2 + 1 - core, far)

    barrier = pltpu.get_barrier_semaphore()

    def greet(i, _):
        pl.semaphore_signal(barrier, inc=1, device_id=(member, peer(i)), device_id_type=MESH)
        return 0

    lax.fori_loop(0, groups - 1, greet, 0)

    n_col = n_lon // LANES

    half = lat_loc // 2

    def f_in(h, x):
        part = pl.ds(h * half, half)
        return pltpu.make_async_copy(f_hbm.at[:, part, pl.ds(x * LANES, LANES)], f_v.at[x, :, part, :], f_sem.at[h, x])

    n_top = groups * rows
    n_low = tf_hbm.shape[0] - n_top
    tf_in = pltpu.make_async_copy(tf_hbm.at[pl.ds(n_low, n_top)], tf_v.at[pl.ds(n_low, n_top)], in_sem.at[0])
    tf_rest = pltpu.make_async_copy(tf_hbm.at[pl.ds(0, n_low)], tf_v.at[pl.ds(0, n_low)], in_sem.at[3])
    ti_in = pltpu.make_async_copy(ti_hbm, ti_v, in_sem.at[1])
    tf_in.start()
    for h in range(2):
        for x in range(n_col):
            f_in(h, x).start()
    tf_rest.start()

    def table_copy(src, dst, sem, k):
        low = k * groups
        return pltpu.make_async_copy(src.at[k * groups + me, pl.ds(low, l_max - low), :], dst.at[k, pl.ds(low, l_max - low), :], sem.at[k])

    n_slot = stage.shape[0]
    w_blk = stage.shape[1] // (2 * n_chan)
    n_blk = l_max // w_blk
    blk_rows = stage.shape[1]

    def w_copy(b, slot):
        return pltpu.make_async_copy(w_hbm.at[pl.ds((n_blk - 1 - b) * blk_rows, blk_rows), :], stage.at[slot], w_sem.at[slot])

    lane = me * lat_loc // LANES * LANES
    pi_loc_in = pltpu.make_async_copy(
        pi_hbm.at[pl.ds(top * piece * groups, piece * groups), pl.ds(top * l_step, l_step), pl.ds(pl.multiple_of(lane, LANES), LANES)],
        pi_loc, in_sem.at[2])

    def start_loads():
        for s in range(n_slot):
            w_copy(s, s).start()
        for k in reversed(range(per_dev)):
            table_copy(pw_hbm, pw_v, pw_sem, k).start()
            if k < top * piece:
                table_copy(pi_hbm, pi_v, pi_sem, k).start()
            low, first = k * groups, (k // piece) * l_step
            if low > first:
                pw_v[k, first:low, :] = jnp.zeros((low - first, n_lat), F32)
                if k < top * piece:
                    pi_v[k, first:low, :] = jnp.zeros((low - first, n_lat), F32)
        pi_loc_in.start()
        ti_in.start()

    tf_in.wait()
    tall = lat_loc + PAD
    f_rows = f_v.reshape(n_col, n_chan * tall, LANES)

    def dft_out(j, u, f_pair):
        r = dot(tf_v[j * groups * rows:(j + 1) * groups * rows, :], f_pair, ((1,), (1,)))
        both = [r[:, e * n_chan:(e + 1) * n_chan].reshape(groups, rows, n_chan) for e in range(2)]
        at = pl.ds(pl.multiple_of(u * 2 * rows, 2 * rows), 2 * rows)
        f_send[j * groups:(j + 1) * groups, at, :] = jnp.concatenate(both, axis=1).astype(BF16)

    def dft_first(u, _):
        pair = []
        for e in range(2):
            here = pl.ds(2 * u + e, n_chan, stride=tall)
            f_t = jnp.concatenate([f_rows[x, here, :] for x in range(n_col)], axis=1)
            f_d[2 * u + e] = f_t
            pair.append(f_t.astype(BF16))
        dft_out(top, u, jnp.concatenate(pair, axis=0))
        return 0

    def dft_next(j, u, _):
        f_pair = jnp.concatenate([f_d[2 * u + e].astype(BF16) for e in range(2)], axis=0)
        dft_out(j, u, f_pair)
        return 0

    def fwd_copy(p, to, slot):
        j, part = (p, pl.ds(0, block)) if p < top else (top, pl.ds(0, block // 2))
        if p == n_chunk:
            part = pl.ds(block // 2, block // 2)
        return pltpu.make_async_remote_copy(
            src_ref=f_send.at[j * groups + to, part], dst_ref=f_recv.at[j * groups + slot, part], send_sem=fs_sem.at[p, to],
            recv_sem=fr_sem.at[p, slot], device_id=(member, to), device_id_type=MESH)

    def back_copy(p, to, slot):
        j, part = (p, pl.ds(0, block)) if p else (0, pl.ds(0, n_first))
        if p == n_chunk:
            j, part = 0, pl.ds(n_first, block - n_first)
        return pltpu.make_async_remote_copy(
            src_ref=g_send.at[j * groups + to, part], dst_ref=g_recv.at[j * groups + slot, part], send_sem=gs_sem.at[p, to],
            recv_sem=gr_sem.at[p, slot], device_id=(member, to), device_id_type=MESH)

    def own_copy(src, dst, j, own):
        return pltpu.make_async_copy(src.at[j * groups + me], dst.at[j * groups + me], own_sem.at[own])

    def send_all(copy, j):
        def go(i, _):
            copy(j, peer(i), me).start()
            return 0

        lax.fori_loop(0, groups - 1, go, 0)

    def recv_all(copy, j):
        def got(i, _):
            s = lax.rem(me + i, groups)
            copy(j, s, s).wait_recv()
            return 0

        lax.fori_loop(1, groups, got, 0)

    def sent_all(copy, j):
        def done(i, _):
            s = lax.rem(me + i, groups)
            copy(j, s, s).wait_send()
            return 0

        lax.fori_loop(1, groups, done, 0)

    n_hop = n_z // 2

    def b_part(h, sgn):
        if h < n_hop:
            return pl.ds(0, b_rows)
        return pl.ds(0 if sgn > 0 else b_rows // 2, b_rows // 2)

    def chip(dz):
        return lax.rem(z + dz + n_z, n_z)

    def b_remote(s, part, to, sems, n):
        return pltpu.make_async_remote_copy(
            src_ref=b_all.at[s, part], dst_ref=b_all.at[s, part], send_sem=sems[0].at[n], recv_sem=sems[1].at[n],
            device_id=(member, to), device_id_type=MESH)

    def hop(h, sgn, arriving):
        s = chip(-sgn * (h if arriving else h - 1)) * 2 + core
        n = (h - 1) * 2 + (sgn < 0)
        return b_remote(s, b_part(h, sgn), chip(sgn) * 2 + core, (hop_s, hop_r), n)

    def sib(h, sgn, arriving):
        s = chip(-sgn * h) * 2 + (1 - core if arriving else core)
        n = 0 if h == 0 else (h - 1) * 2 + (sgn < 0) + 1
        return b_remote(s, b_part(h, sgn), z * 2 + 1 - core, (sib_s, sib_r), n)

    hops = [(h, sgn) for h in range(1, n_hop + 1) for sgn in (1, -1)]

    def relay(h):
        for sgn in (1, -1):
            if h > 0:
                hop(h, sgn, True).wait_recv()
            if h < n_hop:
                hop(h + 1, sgn, False).start()
            if h > 0 or sgn > 0:
                sib(h, sgn, False).start()

    def b_done():
        for h, sgn in hops:
            hop(h, sgn, False).wait_send()
        for h, sgn in [(0, 1)] + hops:
            sib(h, sgn, False).wait_send()

    order = list(reversed(range(n_chunk)))

    def send_fwd(j):
        own_copy(f_send, f_recv, j, j).start()
        send_all(fwd_copy, j)

    def send_back(j):
        own_copy(g_send, g_recv, j, n_chunk + j).start()
        send_all(back_copy, j)
        if j == 0:
            send_all(back_copy, n_chunk)

    for h in range(2):
        for x in range(n_col):
            f_in(h, x).wait()
        if h == 1:
            start_loads()
        lax.fori_loop(h * half // 2, (h + 1) * half // 2, dft_first, 0, unroll=4)
        if h == 0:
            pl.semaphore_wait(barrier, groups - 1)
            send_all(fwd_copy, top)
    own_copy(f_send, f_recv, top, top).start()
    send_all(fwd_copy, n_chunk)
    tf_rest.wait()
    for j in order[1:]:
        lax.fori_loop(0, lat_loc // 2, functools.partial(dft_next, j), 0, unroll=2)
        if j == top - 1:
            send_fwd(j)

    sign = jnp.where(lax.broadcasted_iota(jnp.int32, (rows, n_chan), 0) < piece, -1.0, 1.0).astype(F32)

    def load_w(b, _):
        slot = lax.rem(b, n_slot)
        w_copy(b, slot).wait()
        half = blk_rows // 2
        re = stage[slot, pl.ds(0, half, stride=2), :]
        im = stage[slot, pl.ds(1, half, stride=2), :]
        at = pl.ds(pl.multiple_of((n_blk - 1 - b) * half, half), half)
        w_v[at, :n_chan] = re.astype(BF16)
        w_v[at, n_chan:] = im.astype(BF16)

        @pl.when(b + n_slot < n_blk)
        def _():
            w_copy(b + n_slot, slot).start()

        return 0

    blk_chunk = n_blk // n_chunk
    n_row = n_lat * rows
    for at, j in enumerate(order):
        lax.fori_loop(at * blk_chunk, (at + 1) * blk_chunk, load_w, 0)
        own_copy(f_send, f_recv, j, j).wait()
        recv_all(fwd_copy, j)
        if j == top:
            recv_all(fwd_copy, n_chunk)
        low = j * l_step
        n_l = l_max - low

        def widen(s, _):
            wide[pl.ds(pl.multiple_of(s * block, block), block), :] = f_recv[j * groups + s].astype(F32)
            return 0

        lax.fori_loop(0, groups, widen, 0)
        for i in range(piece):
            k = j * piece + i
            table_copy(pw_hbm, pw_v, pw_sem, k).wait()
            re = wide[pl.ds(i, n_lat, stride=rows), :]
            im = wide[pl.ds(piece + i, n_lat, stride=rows), :]
            spec = jnp.concatenate([re, im], axis=1).astype(BF16)
            a = dot(pw_v[k, low:, :].astype(BF16), spec, ((1,), (0,)))
            coef[pl.ds(low * rows + i, n_l, stride=rows), :] = a[:, :n_chan]
            coef[pl.ds(low * rows + piece + i, n_l, stride=rows), :] = a[:, n_chan:]

        def mix(v, _):
            for e in range(8):
                deg = v * 8 + e
                here = pl.ds(pl.multiple_of(deg * rows, rows), rows)
                w_l = w_v[pl.ds(pl.multiple_of(deg * n_chan, n_chan), n_chan), :]
                r = dot(coef[here, :].astype(BF16), w_l, ((1,), (0,)))
                coef[here, :] = r[:, :n_chan] + sign * pltpu.roll(r[:, n_chan:], piece, 0)
            return 0

        lax.fori_loop(low // 8, l_max // 8, mix, 0)
        if j == top:
            for i in range(piece):
                n_i = heights[i]
                base = (l_max - n_i) * rows
                re = coef[pl.ds(base + i, n_i, stride=rows), :]
                im = coef[pl.ds(base + piece + i, n_i, stride=rows), :]
                b_all[me, starts[i]:starts[i] + n_i, :] = jnp.concatenate([re, im], axis=1).astype(BF16)
            relay(0)
            send_fwd(top - 2)
            continue
        for i in range(piece):
            k = j * piece + i
            table_copy(pi_hbm, pi_v, pi_sem, k).wait()
            re = coef[pl.ds(low * rows + i, n_l, stride=rows), :]
            im = coef[pl.ds(low * rows + piece + i, n_l, stride=rows), :]
            b = jnp.concatenate([re, im], axis=1).astype(BF16)
            g = dot(pi_v[k, low:, :].astype(BF16), b, ((0,), (0,)))
            wide[pl.ds(i, n_lat, stride=rows), :] = g[:, :n_chan]
            wide[pl.ds(piece + i, n_lat, stride=rows), :] = g[:, n_chan:]

        def narrow(s, _):
            g_send[j * groups + s] = wide[pl.ds(pl.multiple_of(s * block, block), block), :].astype(BF16)
            return 0

        lax.fori_loop(0, groups, narrow, 0)
        relay(top - j)
        if j == top - 1:
            send_fwd(0)
        if j == top - 2:
            send_back(top - 1)
        if j == 0:
            send_back(1)
            send_back(0)

    def own_rows(d, _):
        for i in range(piece):
            n_i = heights[i]
            p_i = pltpu.roll(pi_loc[i * groups + d, l_step - n_i:, :], lax.rem(lane + LANES - me * lat_loc, LANES), 1)
            g = dot(p_i.T[:lat_loc].astype(BF16), b_all[d, starts[i]:starts[i] + n_i, :], ((1,), (0,)))
            wide[pl.ds(d * block + i, lat_loc, stride=rows), :] = g[:, :n_chan]
            wide[pl.ds(d * block + piece + i, lat_loc, stride=rows), :] = g[:, n_chan:]
        g_recv[top * groups + d] = wide[pl.ds(pl.multiple_of(d * block, block), block), :].astype(BF16)
        return 0

    ti_in.wait()
    back_order = [top - 1, top] + order[2:]
    for at, j in enumerate(back_order):
        if j == top:
            relay(n_hop)
            for h, sgn in [(0, 1)] + hops:
                sib(h, sgn, True).wait_recv()
            pi_loc_in.wait()
            lax.fori_loop(0, groups, own_rows, 0)
        else:
            own_copy(g_send, g_recv, j, n_chunk + j).wait()
            recv_all(back_copy, j)
        last = at == n_chunk - 1

        def inverse(u, _):
            pair = g_recv[j * groups:(j + 1) * groups, pl.ds(pl.multiple_of(u * 2 * rows, 2 * rows), 2 * rows), :].astype(F32)
            for half in range(2):
                t = 2 * u + half
                g_t = pair[:, half * rows:(half + 1) * rows, :].reshape(groups * rows, n_chan)
                h = dot(g_t.T.astype(BF16), ti_v[j * groups * rows:(j + 1) * groups * rows, :], ((1,), (0,)))
                kept = pl.ds(pl.multiple_of(t * n_chan, n_chan), n_chan)
                for x in range(n_col):
                    lanes = slice(x * LANES, (x + 1) * LANES)
                    h_x = h[:, lanes]
                    if at > 0:
                        h_x = h_x + f_rows[x, kept, :]
                    if last:
                        o_v[x][pl.ds(t, n_chan, stride=tall), :] = f_d[t, :, lanes] + jax.nn.gelu(h_x)
                    else:
                        f_rows[x, kept, :] = h_x
            return 0

        if last:
            first = n_first // rows // 2
            lax.fori_loop(0, first, inverse, 0, unroll=2)
            recv_all(back_copy, n_chunk)
            lax.fori_loop(first, lat_loc // 2, inverse, 0, unroll=2)
        else:
            lax.fori_loop(0, lat_loc // 2, inverse, 0)
    for j in order:
        sent_all(fwd_copy, j)
        if j < top:
            sent_all(back_copy, j)
    b_done()
    sent_all(fwd_copy, n_chunk)
    sent_all(back_copy, n_chunk)


def out_kernel(n_chan, lat_loc, *refs):
    parts, o_hbm, sem = refs[:-2], refs[-2], refs[-1]
    copies = []
    for x, part in enumerate(parts):
        rows = part.reshape(n_chan, part.shape[0] // n_chan, LANES).at[:, pl.ds(0, lat_loc), :]
        copies.append(pltpu.make_async_copy(rows, o_hbm.at[:, :, pl.ds(x * LANES, LANES)], sem.at[x]))
    for copy in copies:
        copy.start()
    for copy in copies:
        copy.wait()


def solution(mesh):
    groups = mesh.shape["lat"]

    def local_layer(field_loc, p_fwd, p_inv, w_mix):
        n_chan, lat_loc, n_lon = field_loc.shape
        l_max, _, n_lat = p_fwd.shape
        per_dev = l_max // groups
        rows = 2 * per_dev // N_CHUNK
        block = lat_loc * rows
        b_rows = sum(l_max - k * groups for k in range(per_dev - per_dev // N_CHUNK, per_dev))
        fwd_tab, inv_tab = wave_tables(n_lon, groups, per_dev, N_CHUNK)
        w_rows = w_mix.transpose(0, 1, 3, 2).reshape(l_max * n_chan * 2, n_chan)
        hbm = pl.BlockSpec(memory_space=pltpu.HBM)
        exchange = pltpu.VMEM((N_CHUNK * groups, block, n_chan), BF16)
        dma = pltpu.SemaphoreType.DMA
        out = pl.pallas_call(
            functools.partial(layer_kernel, (groups, n_chan, lat_loc, n_lon, l_max, n_lat, N_CHUNK)),
            out_shape=[pltpu.VMEM((n_chan * (lat_loc + PAD), LANES), F32)] * (n_lon // LANES),
            in_specs=[hbm] * 6,
            out_specs=[pl.BlockSpec(memory_space=pltpu.VMEM)] * (n_lon // LANES),
            scratch_shapes=[
                pltpu.VMEM((n_lon // LANES, n_chan, lat_loc + PAD, LANES), F32),
                pltpu.VMEM((lat_loc, n_chan, n_lon), F32),
                pltpu.VMEM((l_max * n_chan, 2 * n_chan), BF16),
                pltpu.VMEM((4, 8 * n_chan * 2, n_chan), F32),
                pltpu.VMEM((per_dev, l_max, n_lat), F32),
                pltpu.VMEM((per_dev - per_dev // N_CHUNK, l_max, n_lat), F32),
                exchange, exchange, exchange, exchange,
                pltpu.VMEM((n_lat * rows, n_chan), F32),
                pltpu.VMEM((l_max * rows, n_chan), F32),
                pltpu.VMEM((groups, b_rows, 2 * n_chan), BF16),
                pltpu.VMEM((l_max // N_CHUNK, l_max // N_CHUNK, LANES), F32),
                pltpu.VMEM(fwd_tab.shape, BF16),
                pltpu.VMEM(inv_tab.shape, BF16),
                dma((4,)), dma((2, n_lon // LANES)), dma((per_dev,)), dma((per_dev,)), dma((4,)), dma((2 * N_CHUNK,)),
                dma((N_CHUNK + 1, groups)), dma((N_CHUNK + 1, groups)), dma((N_CHUNK + 1, groups)), dma((N_CHUNK + 1, groups)),
                dma((groups // 2,)), dma((groups // 2,)), dma((groups // 2 + 1,)), dma((groups // 2 + 1,)),
            ],
            compiler_params=pltpu.CompilerParams(collective_id=0, has_side_effects=True, vmem_limit_bytes=56 * 2**20),
            name="spectral_layer",
        )(field_loc, p_fwd, p_inv, w_rows, fwd_tab, inv_tab)
        vmem = pl.BlockSpec(memory_space=pltpu.VMEM)
        return pl.pallas_call(
            functools.partial(out_kernel, n_chan, lat_loc),
            out_shape=jax.ShapeDtypeStruct(field_loc.shape, F32),
            in_specs=[vmem] * len(out),
            out_specs=hbm,
            scratch_shapes=[dma((len(out),))],
            compiler_params=pltpu.CompilerParams(vmem_limit_bytes=2**20),
            name="result_out",
        )(*out)

    return jax.shard_map(local_layer, mesh=mesh, in_specs=(P("member", "lat", None), P(), P(), P()), out_specs=P("member", "lat", None), check_vma=False)
```
